128 devices in a mesh: fsdp: 64 (over z, y, x), ep: 2 (over core).
Axes of the slice: x: 4, y: 4, z: 4, core: 2. Of those that a mesh axis runs over, the one named last changes fastest.
Arguments:
- x_in: bfloat16 [2, 131072, 512], P(None, ('fsdp', 'ep'))
- dy_out: bfloat16 [2, 131072, 512], P(None, ('fsdp', 'ep'))
- expert_idx: int32 [2, 131072, 2], P(None, ('fsdp', 'ep'))
- gate_prob: float32 [2, 131072, 2], P(None, ('fsdp', 'ep'))
- w_one: bfloat16 [8, 512, 1792], P('ep', 'fsdp')
- w_two: bfloat16 [8, 1792, 512], P('ep', None, 'fsdp')
- w_three: bfloat16 [8, 512, 1792], P('ep', 'fsdp')
Outputs:
- output 1: bfloat16 [2, 131072, 512], P(None, ('fsdp', 'ep'))
- output 2: float32 [2, 131072, 2], P(None, ('fsdp', 'ep'))
- output 3: float32 [8, 512, 1792], P('ep', 'fsdp')
- output 4: float32 [8, 1792, 512], P('ep', None, 'fsdp')
- output 5: float32 [8, 512, 1792], P('ep', 'fsdp')
All inputs are finite; a program needn't handle non-finite values.
Results may differ from the reference program's by a relative error of at most 0.00102.
Values are sent between devices in bfloat16 or wider.
A program may use at most 1 GiB of HBM per device.

```python
import jax
import jax.numpy as jnp
from jax import lax

D_MODEL = 512
FF_DIM = 1792
EXPERTS = 8
TOP_K = 2
TOK_DEV = 1024
SOURCES = 128
MICRO_BATCHES = 2
CAPACITY = 320

TOKENS = SOURCES * TOK_DEV
N_CHOICE = TOK_DEV * TOP_K


def draw_routing(key):
    key_hot, key_bias, key_score = jax.random.split(key, 3)
    expert_ids = jnp.arange(EXPERTS, dtype=jnp.int32)
    hot_ids = jax.random.randint(key_hot, (MICRO_BATCHES, SOURCES, 1, 1), 0, EXPERTS)
    forced = jnp.arange(TOK_DEV)[:, None] < CAPACITY
    hot_bonus = jnp.where(expert_ids == hot_ids, 1, 0) * jnp.where(forced, 4096, 512)
    source_bias = jax.random.randint(key_bias, (MICRO_BATCHES, SOURCES, 1, EXPERTS), 0, 512)
    rand_score = jax.random.randint(key_score, (MICRO_BATCHES, SOURCES, TOK_DEV, EXPERTS), 0, 1024)
    total_score = (rand_score + source_bias + hot_bonus) * EXPERTS + expert_ids
    chosen = lax.top_k(total_score, TOP_K)[1]
    return chosen.reshape(MICRO_BATCHES, TOKENS, TOP_K).astype(jnp.int32)


def setup_inputs(seed: int = 0) -> dict:
    key_list = jax.random.split(jax.random.key(seed), 7)
    x_vals = jax.random.normal(key_list[0], (MICRO_BATCHES, TOKENS, D_MODEL), jnp.float32)
    dy_vals = jax.random.normal(key_list[1], (MICRO_BATCHES, TOKENS, D_MODEL), jnp.float32)
    routing = draw_routing(key_list[2])
    gate_vals = jax.random.uniform(key_list[3], (MICRO_BATCHES, TOKENS, TOP_K), jnp.float32, 0.2, 1.0)
    w_one = jax.random.normal(key_list[4], (EXPERTS, D_MODEL, FF_DIM), jnp.float32) * D_MODEL ** -0.5
    w_two = jax.random.normal(key_list[5], (EXPERTS, FF_DIM, D_MODEL), jnp.float32) * FF_DIM ** -0.5
    w_three = jax.random.normal(key_list[6], (EXPERTS, D_MODEL, FF_DIM), jnp.float32) * D_MODEL ** -0.5
    return {'x_in': x_vals.astype(jnp.bfloat16), 'dy_out': dy_vals.astype(jnp.bfloat16), 'expert_idx': routing, 'gate_prob': gate_vals, 'w_one': w_one.astype(jnp.bfloat16), 'w_two': w_two.astype(jnp.bfloat16), 'w_three': w_three.astype(jnp.bfloat16)}


def slot_holder(ids_flat):
    one_hot = (ids_flat[:, None] == jnp.arange(EXPERTS, dtype=jnp.int32)[None, :]).astype(jnp.int32)
    position = jnp.sum((jnp.cumsum(one_hot, axis=0) - one_hot) * one_hot, axis=1)
    choice_slot = jnp.where(position < CAPACITY, ids_flat * CAPACITY + position, EXPERTS * CAPACITY)
    holder = jnp.full((EXPERTS * CAPACITY + 1,), N_CHOICE, jnp.int32)
    holder = holder.at[choice_slot].set(jnp.arange(N_CHOICE, dtype=jnp.int32))
    return holder[:EXPERTS * CAPACITY]


def expert_rows(x_rows, dy_rows, gate_rows, w_a, w_b, w_c):
    h_one = jnp.dot(x_rows, w_a, preferred_element_type=jnp.float32)
    h_three = jnp.dot(x_rows, w_c, preferred_element_type=jnp.float32)
    sigma_one = jax.nn.sigmoid(h_one)
    silu_one = h_one * sigma_one
    act_bf = (silu_one * h_three).astype(jnp.bfloat16)
    y_rows = jnp.dot(act_bf, w_b, preferred_element_type=jnp.float32)
    dg_rows = jnp.sum(dy_rows.astype(jnp.float32) * y_rows, axis=1)
    g_rows = (gate_rows[:, None] * dy_rows.astype(jnp.float32)).astype(jnp.bfloat16)
    d_act = jnp.dot(g_rows, w_b.T, preferred_element_type=jnp.float32)
    dh_three = (d_act * silu_one).astype(jnp.bfloat16)
    dh_one = (d_act * h_three * sigma_one * (1.0 + h_one * (1.0 - sigma_one))).astype(jnp.bfloat16)
    dx_rows = (jnp.dot(dh_one, w_a.T, preferred_element_type=jnp.float32) + jnp.dot(dh_three, w_c.T, preferred_element_type=jnp.float32)).astype(jnp.bfloat16)
    gw_one = jnp.dot(x_rows.T, dh_one, preferred_element_type=jnp.float32)
    gw_two = jnp.dot(act_bf.T, g_rows, preferred_element_type=jnp.float32)
    gw_three = jnp.dot(x_rows.T, dh_three, preferred_element_type=jnp.float32)
    return dx_rows, dg_rows, gw_one, gw_two, gw_three


def reference(x_in, dy_out, expert_idx, gate_prob, w_one, w_two, w_three):
    total_choices = MICRO_BATCHES * TOKENS * TOP_K
    holder = lax.map(slot_holder, expert_idx.reshape(MICRO_BATCHES * SOURCES, N_CHOICE))
    block_base = jnp.arange(MICRO_BATCHES * SOURCES, dtype=jnp.int32)[:, None] * N_CHOICE
    slot_choice = jnp.where(holder < N_CHOICE, holder + block_base, total_choices)
    slot_choice = jnp.transpose(slot_choice.reshape(MICRO_BATCHES, SOURCES, EXPERTS, CAPACITY), (2, 0, 1, 3))
    slot_choice = slot_choice.reshape(EXPERTS, MICRO_BATCHES, SOURCES * CAPACITY)
    zero_row = jnp.zeros((1, D_MODEL), x_in.dtype)
    x_flat = jnp.concatenate([x_in.reshape(MICRO_BATCHES * TOKENS, D_MODEL), zero_row], axis=0)
    dy_flat = jnp.concatenate([dy_out.reshape(MICRO_BATCHES * TOKENS, D_MODEL), zero_row], axis=0)
    gate_flat = jnp.concatenate([gate_prob.reshape(total_choices), jnp.zeros((1,), gate_prob.dtype)])

    def expert_step(scan_state, per_expert):
        dx_acc, dg_acc = scan_state
        w_a, w_b, w_c, choices = per_expert
        grad_one = jnp.zeros((D_MODEL, FF_DIM), jnp.float32)
        grad_two = jnp.zeros((FF_DIM, D_MODEL), jnp.float32)
        grad_three = jnp.zeros((D_MODEL, FF_DIM), jnp.float32)
        for mb_index in range(MICRO_BATCHES):
            pick_ids = choices[mb_index]
            tok_ids = pick_ids // TOP_K
            dx_rows, dg_rows, gw_one, gw_two, gw_three = expert_rows(x_flat[tok_ids], dy_flat[tok_ids], gate_flat[pick_ids], w_a, w_b, w_c)
            dx_acc = dx_acc.at[tok_ids].add(dx_rows.astype(jnp.float32))
            dg_acc = dg_acc.at[pick_ids].set(dg_rows)
            grad_one = grad_one + gw_one
            grad_two = grad_two + gw_two
            grad_three = grad_three + gw_three
        return (dx_acc, dg_acc), (grad_one, grad_two, grad_three)

    start_state = (jnp.zeros((MICRO_BATCHES * TOKENS + 1, D_MODEL), jnp.float32), jnp.zeros((total_choices + 1,), jnp.float32))
    end_state, grad_stack = lax.scan(expert_step, start_state, (w_one, w_two, w_three, slot_choice))
    dx_in = end_state[0][:MICRO_BATCHES * TOKENS].astype(jnp.bfloat16).reshape(MICRO_BATCHES, TOKENS, D_MODEL)
    d_gate = end_state[1][:total_choices].reshape(MICRO_BATCHES, TOKENS, TOP_K)
    return (dx_in, d_gate, grad_stack[0], grad_stack[1], grad_stack[2])
```

```python
import functools

import jax
import jax.numpy as jnp
from jax import lax
from jax.experimental import pallas as pl
from jax.experimental.pallas import tpu as pltpu
from jax.sharding import Mesh, PartitionSpec as P

F32 = jnp.float32
BF16 = jnp.bfloat16
ROW_TILE = 512
COL_TILE = 256


def capacity_of(tok_rows, top_k, experts):
    return 8 * ((5 * tok_rows * top_k + 32 * experts - 1) // (32 * experts))


def route_tables(ids_flat, experts, capacity):
    n_choice = ids_flat.shape[0]
    one_hot = (ids_flat[:, None] == jnp.arange(experts, dtype=jnp.int32)[None, :]).astype(jnp.int32)
    position = jnp.sum((jnp.cumsum(one_hot, axis=0) - one_hot) * one_hot, axis=1)
    choice_slot = jnp.where(position < capacity, ids_flat * capacity + position, experts * capacity)
    holder = jnp.full((experts * capacity + 1,), n_choice, jnp.int32)
    holder = holder.at[choice_slot].set(jnp.arange(n_choice, dtype=jnp.int32))
    return choice_slot, holder[:experts * capacity]


def expert_kernel(ff, first, x_ref, dy_ref, q_ref, w_hbm, wt_hbm, *rest):
    if first:
        dx_ref, dg_ref, gw_hbm, w_v, wt_v, gw_v, xt_v, gt_v, sems = rest
        gin_hbm = None
    else:
        gin_hbm, dx_ref, dg_ref, gw_hbm, w_v, wt_v, gw_v, xt_v, gt_v, sems = rest
    step = pl.program_id(0)

    @pl.when(step == 0)
    def _():
        copies = [pltpu.make_async_copy(w_hbm, w_v, sems.at[0]), pltpu.make_async_copy(wt_hbm, wt_v, sems.at[1])]
        if not first:
            copies.append(pltpu.make_async_copy(gin_hbm, gw_v, sems.at[2]))
        for copy in copies:
            copy.start()
        if first:
            gw_v[...] = jnp.zeros_like(gw_v)
        for copy in copies:
            copy.wait()

    x = x_ref[...]
    dyf = dy_ref[...].astype(F32)
    g = (q_ref[...] * dyf).astype(BF16)
    xt_v[...] = x.T
    gt_v[...] = g.T
    dot = functools.partial(jnp.dot, preferred_element_type=F32)
    y = None
    dx = None
    for lo in range(0, ff, COL_TILE):
        one, two, three = (pl.ds(k * ff + lo, COL_TILE) for k in range(3))
        h_one = dot(x, w_v[:, one])
        h_three = dot(x, w_v[:, three])
        d_act = dot(g, w_v[:, two])
        sigma = jax.nn.sigmoid(h_one)
        silu = h_one * sigma
        act = (silu * h_three).astype(BF16)
        dh_three = (d_act * silu).astype(BF16)
        dh_one = (d_act * h_three * sigma * (1.0 + h_one * (1.0 - sigma))).astype(BF16)
        y_part = dot(act, wt_v[two, :])
        dx_part = dot(dh_one, wt_v[one, :]) + dot(dh_three, wt_v[three, :])
        y = y_part if y is None else y + y_part
        dx = dx_part if dx is None else dx + dx_part
        gw_v[:, one] += dot(xt_v[...], dh_one)
        gw_v[:, three] += dot(xt_v[...], dh_three)
        gw_v[:, two] += dot(gt_v[...], act)
    dg_ref[...] = jnp.sum(dyf * y, axis=1, keepdims=True)
    dx_ref[...] = dx.astype(BF16)

    @pl.when(step == pl.num_programs(0) - 1)
    def _():
        out = pltpu.make_async_copy(gw_v, gw_hbm, sems.at[0])
        out.start()
        out.wait()


def expert_pass(x_rows, dy_rows, gate_rows, w_full, wt_full, grad_in):
    rows, d_model = x_rows.shape
    ff = w_full.shape[1] // 3
    first = grad_in is None
    row_block = pl.BlockSpec((ROW_TILE, d_model), lambda i: (i, 0))
    col_block = pl.BlockSpec((ROW_TILE, 1), lambda i: (i, 0))
    whole = pl.BlockSpec(memory_space=pl.ANY)
    args = [x_rows, dy_rows, gate_rows, w_full, wt_full] + ([] if first else [grad_in])
    in_specs = [row_block, row_block, col_block, whole, whole] + ([] if first else [whole])
    return pl.pallas_call(
        functools.partial(expert_kernel, ff, first),
        grid=(rows // ROW_TILE,),
        in_specs=in_specs,
        out_specs=[row_block, col_block, whole],
        out_shape=[
            jax.ShapeDtypeStruct((rows, d_model), BF16),
            jax.ShapeDtypeStruct((rows, 1), F32),
            jax.ShapeDtypeStruct((d_model, 3 * ff), F32),
        ],
        scratch_shapes=[
            pltpu.VMEM((d_model, 3 * ff), BF16),
            pltpu.VMEM((3 * ff, d_model), BF16),
            pltpu.VMEM((d_model, 3 * ff), F32),
            pltpu.VMEM((d_model, ROW_TILE), BF16),
            pltpu.VMEM((d_model, ROW_TILE), BF16),
            pltpu.SemaphoreType.DMA((3,)),
        ],
        compiler_params=pltpu.CompilerParams(vmem_limit_bytes=60 * 2**20),
        cost_estimate=pl.CostEstimate(flops=18 * rows * d_model * ff, bytes_accessed=40 * 2**20, transcendentals=2 * rows * ff),
        name='expert_first' if first else 'expert_next',
    )(*args)


def solution(mesh):
    side = round(mesh.shape['fsdp'] ** (1 / 3))
    cores = mesh.shape['ep']
    grid_mesh = Mesh(mesh.devices.reshape(side, side, side, cores), ('z', 'y', 'x', 'c'))
    tok_spec = P(None, ('z', 'y', 'x', 'c'), None)
    spec_edf = P('c', ('z', 'y', 'x'), None)
    spec_efd = P('c', None, ('z', 'y', 'x'))
    ring = ('x', 'c')

    def local_step(x_in, dy_out, expert_idx, gate_prob, w_one, w_two, w_three):
        micro_count, tok_rows, d_model = x_in.shape
        top_k = expert_idx.shape[2]
        local_experts, shard, ff = w_one.shape
        experts = local_experts * cores
        capacity = capacity_of(tok_rows, top_k, experts)
        n_choice = tok_rows * top_k
        rows = experts * capacity
        w_cat = jnp.concatenate([w_one, jnp.transpose(w_two, (0, 2, 1)), w_three], axis=2)
        w_mine = lax.all_to_all(w_cat, 'x', 0, 0, tiled=True).reshape(local_experts * shard, 3 * ff)
        w_full = lax.all_gather(w_mine, ('z', 'y'), axis=0, tiled=True)
        wt_full = w_full.T
        zero_row = jnp.zeros((1, d_model), x_in.dtype)
        zero_val = jnp.zeros((1,), F32)
        send_shape = (experts, capacity)
        sent = []
        for mb_index in range(micro_count):
            ids = expert_idx[mb_index].reshape(n_choice)
            owner = (ids % local_experts) * cores + ids // local_experts
            choice_slot, holder = route_tables(owner, experts, capacity)
            tok_slot = holder // top_k
            x_send = jnp.concatenate([x_in[mb_index], zero_row], axis=0)[tok_slot]
            dy_send = jnp.concatenate([dy_out[mb_index], zero_row], axis=0)[tok_slot]
            gate_send = jnp.concatenate([gate_prob[mb_index].reshape(n_choice), zero_val])[holder]
            x_rows = lax.all_to_all(x_send.reshape(send_shape + (d_model,)), ring, 0, 0, tiled=True)
            dy_rows = lax.all_to_all(dy_send.reshape(send_shape + (d_model,)), ring, 0, 0, tiled=True)
            gate_rows = lax.all_to_all(gate_send.reshape(send_shape), ring, 0, 0, tiled=True)
            sent.append((choice_slot, x_rows, dy_rows, gate_rows))
        dx_parts = []
        dg_parts = []
        grad_sum = None
        for choice_slot, x_rows, dy_rows, gate_rows in sent:
            dx_rows, dg_rows, grad_sum = expert_pass(x_rows.reshape(rows, d_model), dy_rows.reshape(rows, d_model), gate_rows.reshape(rows, 1), w_full, wt_full, grad_sum)
            dx_back = lax.all_to_all(dx_rows.reshape(send_shape + (d_model,)), ring, 0, 0, tiled=True).reshape(rows, d_model)
            dg_back = lax.all_to_all(dg_rows.reshape(send_shape), ring, 0, 0, tiled=True).reshape(rows)
            picked = jnp.concatenate([dx_back, zero_row], axis=0)[choice_slot].reshape(tok_rows, top_k, d_model)
            dx_parts.append(jnp.sum(picked.astype(F32), axis=1).astype(BF16))
            dg_parts.append(jnp.concatenate([dg_back, zero_val])[choice_slot].reshape(tok_rows, top_k))
        dw_mine = lax.psum_scatter(grad_sum, ('z', 'y'), scatter_dimension=0, tiled=True)
        dw_all = lax.all_to_all(dw_mine.reshape(local_experts, shard, 3 * ff), 'x', 0, 0, tiled=True)
        dw_one, dw_two, dw_three = dw_all[:, :, :ff], jnp.transpose(dw_all[:, :, ff:2 * ff], (0, 2, 1)), dw_all[:, :, 2 * ff:]
        return jnp.stack(dx_parts), jnp.stack(dg_parts), dw_one, dw_two, dw_three

    return jax.shard_map(local_step, mesh=grid_mesh, in_specs=(tok_spec, tok_spec, tok_spec, tok_spec, spec_edf, spec_efd, spec_edf), out_specs=(tok_spec, tok_spec, spec_edf, spec_efd, spec_edf), check_vma=False)
```

```python
import functools

import jax
import jax.numpy as jnp
from jax import lax
from jax.experimental import pallas as pl
from jax.experimental.pallas import tpu as pltpu
from jax.sharding import Mesh, PartitionSpec as P


F32 = jnp.float32
BF16 = jnp.bfloat16
UNIT = 16
COL_TILE = 256
NT_DIMS = (((1,),(1,)),((),()))


def row_pieces(n_sm, cap, emit):
    off = jnp.int32(0)
    for s in range(n_sm.shape[0]):
        n = n_sm[s]
        for k in range(cap // 64):
            @pl.when((k + 1) * 4 <= n)
            def _(k=k, s=s, off=off):
                emit(s * cap + k * 64, off * UNIT + k * 64, 64)
        base = (n // 4) * 4

        @pl.when((n // 2) % 2 == 1)
        def _(s=s, off=off, base=base):
            emit(s * cap + base * UNIT, (off + base) * UNIT, 32)

        tail = (n // 2) * 2

        @pl.when(n % 2 == 1)
        def _(s=s, off=off, tail=tail):
            emit(s * cap + tail * UNIT, (off + tail) * UNIT, 16)

        off = off + n
    return off


def expert_kernel(ff, cap, first, n_sm, xdy_hbm, q_ref, w_hbm, *rest):
    if first:
        dx_hbm, dg_ref, gw_hbm, xdy_v, q_v, dg_v, dx_v, w_v, gw_v, xt_v, gt_v, sems = rest
        gin_hbm = gin_v = None
    else:
        gin_hbm, dx_hbm, dg_ref, gw_hbm, xdy_v, q_v, dg_v, dx_v, w_v, gw_v, xt_v, gt_v, gin_v, sems = rest
    d = w_hbm.shape[0]
    n_src = n_sm.shape[0]

    def m8(v, n=UNIT):
        return v if isinstance(v, int) else pl.multiple_of(v, n)

    def fetch(slot, packed, size):
        return pltpu.make_async_copy(xdy_hbm.at[pl.ds(m8(slot), size)], xdy_v.at[pl.ds(m8(packed), size)], sems.at[0])

    units = row_pieces(n_sm, cap, lambda *a: fetch(*a).start())
    parts = [pltpu.make_async_copy(w_hbm.at[:, pl.ds(k * ff, ff)], w_v.at[:, pl.ds(k * ff, ff)], sems.at[1 + k]) for k in range(3)]
    for p in parts:
        p.start()
    if not first:
        gin = pltpu.make_async_copy(gin_hbm, gin_v, sems.at[4])
        gin.start()
    gw_v[...] = jnp.zeros_like(gw_v)
    q_cols = q_ref[...].T
    off = jnp.int32(0)
    for s in range(n_src):
        q_v[pl.ds(pl.multiple_of(off * UNIT, UNIT), cap), :] = q_cols[:, s:s + 1]
        off = off + n_sm[s]
    q_v[pl.ds(pl.multiple_of(off * UNIT, UNIT), 512), :] = jnp.zeros((512, 1), F32)

    def clear(i, c):
        xdy_v[pl.ds(pl.multiple_of(i * UNIT, UNIT), UNIT), :] = jnp.zeros((UNIT, 2 * d), BF16)
        return c

    lax.fori_loop(units, ((units + 15) // 16) * 16, clear, 0)
    row_pieces(n_sm, cap, lambda *a: fetch(*a).wait())
    for p in parts:
        p.wait()

    dot = functools.partial(jnp.dot, preferred_element_type=F32)
    dot_nt = lambda a, b: lax.dot_general(a, b, NT_DIMS, preferred_element_type=F32)

    def tile(lo_row, rt):
        rows = pl.ds(pl.multiple_of(lo_row, 256), rt)
        x = xdy_v[rows, :d]
        dy = xdy_v[rows, d:]
        g = (q_v[rows, :] * dy.astype(F32)).astype(BF16)
        xt_v[:, :rt] = x.T
        gt_v[:, :rt] = g.T
        y = None
        dx = None
        for lo in range(0, ff, COL_TILE):
            one, two, three = (pl.ds(k * ff + lo, COL_TILE) for k in range(3))
            h_one = dot(x, w_v[:, one])
            h_three = dot(x, w_v[:, three])
            d_act = dot(g, w_v[:, two])
            sigma = jax.nn.sigmoid(h_one)
            silu = h_one * sigma
            act = (silu * h_three).astype(BF16)
            dh_three = (d_act * silu).astype(BF16)
            dh_one = (d_act * h_three * sigma * (1.0 + h_one * (1.0 - sigma))).astype(BF16)
            y_part = dot_nt(act, w_v[:, two])
            dx_part = dot_nt(dh_one, w_v[:, one]) + dot_nt(dh_three, w_v[:, three])
            y = y_part if y is None else y + y_part
            dx = dx_part if dx is None else dx + dx_part
            gw_v[:, one] += dot(xt_v[:, :rt], dh_one)
            gw_v[:, three] += dot(xt_v[:, :rt], dh_three)
            gw_v[:, two] += dot(gt_v[:, :rt], act)
        dg_v[rows, :] = jnp.sum(dy.astype(F32) * y, axis=1, keepdims=True)
        dx_v[rows, :] = dx.astype(BF16)

    total = units * UNIT
    full = (total + 255) // 512

    def big(i, c):
        tile(i * 512, 512)
        return c

    lax.fori_loop(0, full, big, 0)

    @pl.when(full * 512 < total)
    def _():
        tile(full * 512, 256)

    if not first:
        gin.wait()
    outs = []
    for k in range(3):
        cols = pl.ds(k * ff, ff)
        if not first:
            gw_v[:, cols] += gin_v[:, cols]
        o = pltpu.make_async_copy(gw_v.at[:, cols], gw_hbm.at[:, cols], sems.at[1 + k])
        o.start()
        outs.append(o)

    def put(slot, packed, size):
        return pltpu.make_async_copy(dx_v.at[pl.ds(m8(packed), size)], dx_hbm.at[pl.ds(m8(slot), size)], sems.at[0])

    row_pieces(n_sm, cap, lambda *a: put(*a).start())
    off = jnp.int32(0)
    cols = []
    for s in range(n_src):
        cols.append(dg_v[pl.ds(pl.multiple_of(off * UNIT, UNIT), cap), :])
        off = off + n_sm[s]
    dg_ref[...] = jnp.concatenate(cols, axis=1).T
    row_pieces(n_sm, cap, lambda *a: put(*a).wait())
    for o in outs:
        o.wait()


def expert_pass(n_units, xdy, gates, w_full, grad_in):
    rows, d2 = xdy.shape
    d = d2 // 2
    ff = w_full.shape[1] // 3
    cap = gates.shape[1]
    first = grad_in is None
    whole = pl.BlockSpec(memory_space=pl.ANY)
    vm = pl.BlockSpec(memory_space=pltpu.VMEM)
    args = [n_units, xdy, gates, w_full] + ([] if first else [grad_in])
    in_specs = [pl.BlockSpec(memory_space=pltpu.SMEM), whole, vm, whole] + ([] if first else [whole])
    pad = rows + 512
    scratch = [
        pltpu.VMEM((rows, d2), BF16), pltpu.VMEM((pad, 1), F32), pltpu.VMEM((pad, 1), F32), pltpu.VMEM((rows, d), BF16),
        pltpu.VMEM((d, 3 * ff), BF16), pltpu.VMEM((d, 3 * ff), F32), pltpu.VMEM((d, 512), BF16), pltpu.VMEM((d, 512), BF16)]
    if not first:
        scratch.append(pltpu.VMEM((d, 3 * ff), F32))
    scratch.append(pltpu.SemaphoreType.DMA((5,)))
    return pl.pallas_call(
        functools.partial(expert_kernel, ff, cap, first),
        in_specs=in_specs, out_specs=[whole, vm, whole],
        out_shape=[jax.ShapeDtypeStruct((rows, d), BF16), jax.ShapeDtypeStruct(gates.shape, F32), jax.ShapeDtypeStruct((d, 3 * ff), F32)],
        scratch_shapes=scratch,
        compiler_params=pltpu.CompilerParams(vmem_limit_bytes=60 * 2**20),
        cost_estimate=pl.CostEstimate(flops=18 * rows * d * ff, bytes_accessed=40 * 2**20, transcendentals=2 * rows * ff),
        name='expert_first' if first else 'expert_next')(*args)


def capacity_of(tok_rows, top_k, experts):
    return 8 * ((5 * tok_rows * top_k + 32 * experts - 1) // (32 * experts))


def positions(own_ref, owners):
    tokens = own_ref.shape[1]
    who = lax.broadcasted_iota(jnp.int32, (owners, tokens), 0)
    chosen = (own_ref[0:1, :] == who) | (own_ref[1:2, :] == who)
    before = lax.broadcasted_iota(jnp.int32, (tokens, tokens), 0) < lax.broadcasted_iota(jnp.int32, (tokens, tokens), 1)
    flags = jnp.where(chosen, 1.0, 0.0).astype(BF16)
    place = jnp.dot(flags, jnp.where(before, 1.0, 0.0).astype(BF16), preferred_element_type=F32)
    return jnp.where(chosen, place, -1.0)


def dispatch_kernel(owners, cap, own_ref, x_ref, dy_ref, xdy_ref, pos_v):
    step = pl.program_id(0)
    d = x_ref.shape[1]

    @pl.when(step == 0)
    def _():
        pos_v[...] = positions(own_ref, owners)

    place = pos_v[pl.ds(step, 1), :].astype(jnp.int32)
    hit = place == lax.broadcasted_iota(jnp.int32, (cap, place.shape[1]), 0)
    pick = jnp.where(hit, 1.0, 0.0).astype(BF16)
    xdy_ref[:, :d] = jnp.dot(pick, x_ref[...], preferred_element_type=F32).astype(BF16)
    xdy_ref[:, d:] = jnp.dot(pick, dy_ref[...], preferred_element_type=F32).astype(BF16)


def dispatch(own_t, x_in, dy_out, mb, owners, cap):
    _, tokens, d = x_in.shape
    part = pl.BlockSpec((None, tokens, d), lambda i: (mb, 0, 0))
    return pl.pallas_call(
        functools.partial(dispatch_kernel, owners, cap),
        grid=(owners,),
        in_specs=[pl.BlockSpec((None, 2, tokens), lambda i: (mb, 0, 0)), part, part],
        out_specs=pl.BlockSpec((cap, 2 * d), lambda i: (i, 0)),
        out_shape=jax.ShapeDtypeStruct((owners * cap, 2 * d), BF16),
        scratch_shapes=[pltpu.VMEM((owners, tokens), F32)],
        compiler_params=pltpu.CompilerParams(vmem_limit_bytes=60 * 2**20),
        cost_estimate=pl.CostEstimate(flops=4 * owners * cap * tokens * d, bytes_accessed=8 * 2**20, transcendentals=0))(own_t, x_in, dy_out)


def gates_kernel(cap, here_sm, table_ref, gate_ref, cols_v):
    blocks, tokens = table_ref.shape[0], table_ref.shape[2]
    here = here_sm[0].astype(F32)
    first = jnp.concatenate([table_ref[k, 0:1, :] for k in range(blocks)], axis=0) == here
    second = jnp.concatenate([table_ref[k, 1:2, :] for k in range(blocks)], axis=0) == here
    before = lax.broadcasted_iota(jnp.int32, (tokens, tokens), 0) < lax.broadcasted_iota(jnp.int32, (tokens, tokens), 1)
    flags = jnp.where(first | second, 1.0, 0.0).astype(BF16)
    place = jnp.dot(flags, jnp.where(before, 1.0, 0.0).astype(BF16), preferred_element_type=F32)
    place = jnp.where(first | second, place, -1.0).astype(jnp.int32)
    iota = lax.broadcasted_iota(jnp.int32, (cap, tokens), 0)
    cols_v[...] = jnp.zeros_like(cols_v)
    for k in range(blocks):
        gate = jnp.where(first[k:k + 1, :], table_ref[k, 2:3, :], table_ref[k, 3:4, :])
        cols_v[:, k:k + 1] = jnp.sum(jnp.where(place[k:k + 1, :] == iota, gate, 0.0), axis=1, keepdims=True)
    gate_ref[...] = cols_v[...].T[:blocks, :]


def slot_gates(here, table, cap):
    blocks, _, _ = table.shape
    vm = pl.BlockSpec(memory_space=pltpu.VMEM)
    return pl.pallas_call(
        functools.partial(gates_kernel, cap),
        in_specs=[pl.BlockSpec(memory_space=pltpu.SMEM), vm],
        out_specs=vm,
        out_shape=jax.ShapeDtypeStruct((blocks, cap), F32),
        scratch_shapes=[pltpu.VMEM((cap, 128), F32)],
        cost_estimate=pl.CostEstimate(flops=10 * 2**30, bytes_accessed=2**20, transcendentals=0),
        name='slot_gates')(here, table)


def combine_kernel(owners, cap, n_sm, own_ref, back_ref, dg_ref, dx_ref, dgate_ref, rows_v):
    tokens = own_ref.shape[1]
    d = back_ref.shape[1]
    pos = positions(own_ref, owners)
    dg_cols = dg_ref[...].T
    place_iota = lax.broadcasted_iota(jnp.int32, (cap, tokens), 0)
    row_iota = lax.broadcasted_iota(jnp.int32, (cap, d), 0)
    dgate = [jnp.zeros((1, tokens), F32), jnp.zeros((1, tokens), F32)]
    slot = [jnp.full((1, tokens), -1, jnp.int32), jnp.full((1, tokens), -1, jnp.int32)]
    for k in range(owners):
        place = pos[k:k + 1, :].astype(jnp.int32)
        got = jnp.sum(jnp.where(place == place_iota, dg_cols[:, k:k + 1], 0.0), axis=0, keepdims=True)
        kept = jnp.where(place < cap, place + k * cap, -1)
        for j in range(2):
            mine = own_ref[j:j + 1, :] == k
            dgate[j] = jnp.where(mine, got, dgate[j])
            slot[j] = jnp.where(mine, kept, slot[j])
        rows = back_ref[k * cap:(k + 1) * cap, :].astype(F32)
        rows_v[k * cap:(k + 1) * cap, :] = jnp.where(row_iota < n_sm[k], rows, 0.0).astype(BF16)
    dgate_ref[0:1, :] = dgate[0]
    dgate_ref[1:2, :] = dgate[1]
    slots = jnp.concatenate([s.astype(F32) for s in slot] + [jnp.zeros((6, tokens), F32)], axis=0).T.astype(jnp.int32)
    step = 256
    for lo in range(0, tokens, step):
        iota = lax.broadcasted_iota(jnp.int32, (step, owners * cap), 1)
        hit = (slots[lo:lo + step, 0:1] == iota) | (slots[lo:lo + step, 1:2] == iota)
        pick = jnp.where(hit, 1.0, 0.0).astype(BF16)
        dx_ref[lo:lo + step, :] = jnp.dot(pick, rows_v[...], preferred_element_type=F32).astype(BF16)


def combine(n_kept, own_t, back, dg_back, mb, cap):
    rows, d = back.shape
    owners = n_kept.shape[0]
    tokens = own_t.shape[2]
    vm = pl.BlockSpec(memory_space=pltpu.VMEM)
    return pl.pallas_call(
        functools.partial(combine_kernel, owners, cap),
        grid=(1,),
        in_specs=[pl.BlockSpec(memory_space=pltpu.SMEM), pl.BlockSpec((None, 2, tokens), lambda i: (mb, 0, 0)), vm, vm],
        out_specs=[vm, vm],
        out_shape=[jax.ShapeDtypeStruct((tokens, d), BF16), jax.ShapeDtypeStruct((2, tokens), F32)],
        scratch_shapes=[pltpu.VMEM((rows, d), BF16)],
        compiler_params=pltpu.CompilerParams(vmem_limit_bytes=60 * 2**20),
        cost_estimate=pl.CostEstimate(flops=2 * rows * tokens * d, bytes_accessed=6 * 2**20, transcendentals=0))(n_kept, own_t, back, dg_back)


def solution(mesh):
    side = round(mesh.shape['fsdp'] ** (1 / 3))
    cores = mesh.shape['ep']
    grid_mesh = Mesh(mesh.devices.reshape(side, side, side, cores), ('z', 'y', 'x', 'c'))
    tok_spec = P(None, ('z', 'y', 'x', 'c'), None)
    spec_edf = P('c', ('z', 'y', 'x'), None)
    spec_efd = P('c', None, ('z', 'y', 'x'))
    ring = ('x', 'c')

    def local_step(x_in, dy_out, expert_idx, gate_prob, w_one, w_two, w_three):
        micro_count, tok_rows, d_model = x_in.shape
        top_k = expert_idx.shape[2]
        local_experts, shard, ff = w_one.shape
        experts = local_experts * cores
        cap = capacity_of(tok_rows, top_k, experts)
        rows = experts * cap
        ids_t = jnp.transpose(expert_idx, (0, 2, 1))
        own_t = (ids_t % local_experts) * cores + ids_t // local_experts
        q_t = jnp.transpose(gate_prob, (0, 2, 1))
        here = lax.axis_index('x') * cores + lax.axis_index('c')
        table = lax.all_gather(jnp.concatenate([own_t.astype(F32), q_t], axis=1), ring, axis=1)
        table = table.reshape(micro_count * experts, 2 * top_k, tok_rows)
        n_here = jnp.sum((table[:, :top_k] == here.astype(F32)).astype(jnp.int32), axis=(1, 2))
        n_recv = ((jnp.minimum(n_here, cap) + UNIT - 1) // UNIT).reshape(micro_count, experts)
        picks = (own_t[:, :, :, None] == jnp.arange(experts, dtype=jnp.int32)).astype(jnp.int32)
        n_kept = jnp.minimum(jnp.sum(picks, axis=(1, 2)), cap)
        w_cat = jnp.concatenate([w_one, jnp.transpose(w_two, (0, 2, 1)), w_three], axis=2)
        x_id = lax.axis_index('x')
        dealt = [lax.dynamic_index_in_dim(w_cat, x_id, 0, keepdims=False)]
        for k in range(1, local_experts):
            piece = lax.dynamic_index_in_dim(w_cat, (x_id + k) % local_experts, 0, keepdims=False)
            dealt.append(lax.ppermute(piece, 'x', [(i, (i + k) % local_experts) for i in range(local_experts)]))
        slabs = []
        for j in range(local_experts):
            back = (x_id - j) % local_experts
            slab = dealt[0]
            for k in range(1, local_experts):
                slab = jnp.where(back == k, dealt[k], slab)
            slabs.append(slab)
        w_mine = jnp.concatenate(slabs, axis=0)
        w_full = lax.all_gather(w_mine, ('z', 'y'), axis=0, tiled=True)
        xdy = []
        for mb in range(micro_count):
            send = dispatch(own_t, x_in, dy_out, mb, experts, cap)
            xdy.append(lax.all_to_all(send.reshape(experts, cap, 2 * d_model), ring, 0, 0, tiled=True).reshape(rows, 2 * d_model))
        gate_rows = slot_gates(here.reshape(1), table, cap).reshape(micro_count, experts, cap)
        dx_back = []
        dg_rows = []
        grad_sum = None
        for mb in range(micro_count):
            dx_rows, dg, grad_sum = expert_pass(n_recv[mb], xdy[mb], gate_rows[mb], w_full, grad_sum)
            dx_back.append(lax.all_to_all(dx_rows.reshape(experts, cap, d_model), ring, 0, 0, tiled=True).reshape(rows, d_model))
            dg_rows.append(dg)
        dw_mine = lax.psum_scatter(grad_sum, ('z', 'y'), scatter_dimension=0, tiled=True)
        dg_back = lax.all_to_all(jnp.stack(dg_rows, axis=1), ring, 0, 0, tiled=True)
        parts = []
        for mb in range(micro_count):
            parts.append(combine(n_kept[mb], own_t, dx_back[mb], dg_back[:, mb], mb, cap))
        dx_in = jnp.stack([p[0] for p in parts])
        d_gate = jnp.transpose(jnp.stack([p[1] for p in parts]), (0, 2, 1))
        dw_all = lax.all_to_all(dw_mine.reshape(local_experts, shard, 3 * ff), 'x', 0, 0, tiled=True)
        dw_one, dw_two, dw_three = dw_all[:, :, :ff], jnp.transpose(dw_all[:, :, ff:2 * ff], (0, 2, 1)), dw_all[:, :, 2 * ff:]
        return dx_in, d_gate, dw_one, dw_two, dw_three

    return jax.shard_map(local_step, mesh=grid_mesh, in_specs=(tok_spec, tok_spec, tok_spec, tok_spec, spec_edf, spec_efd, spec_edf), out_specs=(tok_spec, tok_spec, spec_edf, spec_efd, spec_edf), check_vma=False)
```

```python
import functools

import jax
import jax.numpy as jnp
from jax import lax
from jax.experimental import pallas as pl
from jax.experimental.pallas import tpu as pltpu
from jax.sharding import Mesh, PartitionSpec as P


F32 = jnp.float32
BF16 = jnp.bfloat16
UNIT = 16
COL_TILE = 256
NT_DIMS = (((1,),(1,)),((),()))


def row_pieces(n_sm, cap, emit):
    off = jnp.int32(0)
    for s in range(n_sm.shape[0]):
        n = n_sm[s]
        for k in range(cap // 64):
            @pl.when((k + 1) * 4 <= n)
            def _(k=k, s=s, off=off):
                emit(s * cap + k * 64, off * UNIT + k * 64, 64)
        base = (n // 4) * 4

        @pl.when((n // 2) % 2 == 1)
        def _(s=s, off=off, base=base):
            emit(s * cap + base * UNIT, (off + base) * UNIT, 32)

        tail = (n // 2) * 2

        @pl.when(n % 2 == 1)
        def _(s=s, off=off, tail=tail):
            emit(s * cap + tail * UNIT, (off + tail) * UNIT, 16)

        off = off + n
    return off


def expert_kernel(ff, cap, first, n_sm, xdy_hbm, q_ref, w_hbm, *rest):
    if first:
        dx_hbm, dg_ref, gw_hbm, xdy_v, q_v, dg_v, dx_v, w_v, gw_v, xt_v, gt_v, sems = rest
        gin_hbm = gin_v = None
    else:
        gin_hbm, dx_hbm, dg_ref, gw_hbm, xdy_v, q_v, dg_v, dx_v, w_v, gw_v, xt_v, gt_v, gin_v, sems = rest
    d = w_hbm.shape[0]
    n_src = n_sm.shape[0]

    def m8(v, n=UNIT):
        return v if isinstance(v, int) else pl.multiple_of(v, n)

    def fetch(slot, packed, size):
        return pltpu.make_async_copy(xdy_hbm.at[pl.ds(m8(slot), size)], xdy_v.at[pl.ds(m8(packed), size)], sems.at[0])

    units = row_pieces(n_sm, cap, lambda *a: fetch(*a).start())
    parts = [pltpu.make_async_copy(w_hbm.at[:, pl.ds(k * ff, ff)], w_v.at[:, pl.ds(k * ff, ff)], sems.at[1 + k]) for k in range(3)]
    for p in parts:
        p.start()
    if not first:
        gin = pltpu.make_async_copy(gin_hbm, gin_v, sems.at[4])
        gin.start()
    gw_v[...] = jnp.zeros_like(gw_v)
    q_cols = q_ref[...].T
    off = jnp.int32(0)
    for s in range(n_src):
        q_v[pl.ds(pl.multiple_of(off * UNIT, UNIT), cap), :] = q_cols[:, s:s + 1]
        off = off + n_sm[s]
    q_v[pl.ds(pl.multiple_of(off * UNIT, UNIT), 512), :] = jnp.zeros((512, 1), F32)

    def clear(i, c):
        xdy_v[pl.ds(pl.multiple_of(i * UNIT, UNIT), UNIT), :] = jnp.zeros((UNIT, 2 * d), BF16)
        return c

    lax.fori_loop(units, ((units + 15) // 16) * 16, clear, 0)
    row_pieces(n_sm, cap, lambda *a: fetch(*a).wait())
    for p in parts:
        p.wait()

    dot = functools.partial(jnp.dot, preferred_element_type=F32)
    dot_nt = lambda a, b: lax.dot_general(a, b, NT_DIMS, preferred_element_type=F32)

    def tile(lo_row, rt):
        rows = pl.ds(pl.multiple_of(lo_row, 256), rt)
        x = xdy_v[rows, :d]
        dy = xdy_v[rows, d:]
        g = (q_v[rows, :] * dy.astype(F32)).astype(BF16)
        xt_v[:, :rt] = x.T
        gt_v[:, :rt] = g.T
        y = None
        dx = None
        for lo in range(0, ff, COL_TILE):
            one, two, three = (pl.ds(k * ff + lo, COL_TILE) for k in range(3))
            h_one = dot(x, w_v[:, one])
            h_three = dot(x, w_v[:, three])
            d_act = dot(g, w_v[:, two])
            sigma = jax.nn.sigmoid(h_one)
            silu = h_one * sigma
            act = (silu * h_three).astype(BF16)
            dh_three = (d_act * silu).astype(BF16)
            dh_one = (d_act * h_three * sigma * (1.0 + h_one * (1.0 - sigma))).astype(BF16)
            y_part = dot_nt(act, w_v[:, two])
            dx_part = dot_nt(dh_one, w_v[:, one]) + dot_nt(dh_three, w_v[:, three])
            y = y_part if y is None else y + y_part
            dx = dx_part if dx is None else dx + dx_part
            gw_v[:, one] += dot(xt_v[:, :rt], dh_one)
            gw_v[:, three] += dot(xt_v[:, :rt], dh_three)
            gw_v[:, two] += dot(gt_v[:, :rt], act)
        dg_v[rows, :] = jnp.sum(dy.astype(F32) * y, axis=1, keepdims=True)
        dx_v[rows, :] = dx.astype(BF16)

    total = units * UNIT
    full = (total + 255) // 512

    def big(i, c):
        tile(i * 512, 512)
        return c

    lax.fori_loop(0, full, big, 0)

    @pl.when(full * 512 < total)
    def _():
        tile(full * 512, 256)

    if not first:
        gin.wait()
    outs = []
    for k in range(3):
        cols = pl.ds(k * ff, ff)
        if not first:
            gw_v[:, cols] += gin_v[:, cols]
        o = pltpu.make_async_copy(gw_v.at[:, cols], gw_hbm.at[:, cols], sems.at[1 + k])
        o.start()
        outs.append(o)

    def put(slot, packed, size):
        return pltpu.make_async_copy(dx_v.at[pl.ds(m8(packed), size)], dx_hbm.at[pl.ds(m8(slot), size)], sems.at[0])

    row_pieces(n_sm, cap, lambda *a: put(*a).start())
    off = jnp.int32(0)
    cols = []
    for s in range(n_src):
        cols.append(dg_v[pl.ds(pl.multiple_of(off * UNIT, UNIT), cap), :])
        off = off + n_sm[s]
    dg_ref[...] = jnp.concatenate(cols, axis=1).T
    row_pieces(n_sm, cap, lambda *a: put(*a).wait())
    for o in outs:
        o.wait()


def expert_pass(n_units, xdy, gates, w_full, grad_in):
    rows, d2 = xdy.shape
    d = d2 // 2
    ff = w_full.shape[1] // 3
    cap = gates.shape[1]
    first = grad_in is None
    whole = pl.BlockSpec(memory_space=pl.ANY)
    vm = pl.BlockSpec(memory_space=pltpu.VMEM)
    args = [n_units, xdy, gates, w_full] + ([] if first else [grad_in])
    in_specs = [pl.BlockSpec(memory_space=pltpu.SMEM), whole, vm, whole] + ([] if first else [whole])
    pad = rows + 512
    scratch = [
        pltpu.VMEM((rows, d2), BF16), pltpu.VMEM((pad, 1), F32), pltpu.VMEM((pad, 1), F32), pltpu.VMEM((rows, d), BF16),
        pltpu.VMEM((d, 3 * ff), BF16), pltpu.VMEM((d, 3 * ff), F32), pltpu.VMEM((d, 512), BF16), pltpu.VMEM((d, 512), BF16)]
    if not first:
        scratch.append(pltpu.VMEM((d, 3 * ff), F32))
    scratch.append(pltpu.SemaphoreType.DMA((5,)))
    return pl.pallas_call(
        functools.partial(expert_kernel, ff, cap, first),
        in_specs=in_specs, out_specs=[whole, vm, whole],
        out_shape=[jax.ShapeDtypeStruct((rows, d), BF16), jax.ShapeDtypeStruct(gates.shape, F32), jax.ShapeDtypeStruct((d, 3 * ff), F32)],
        scratch_shapes=scratch,
        compiler_params=pltpu.CompilerParams(vmem_limit_bytes=60 * 2**20),
        cost_estimate=pl.CostEstimate(flops=18 * rows * d * ff, bytes_accessed=40 * 2**20, transcendentals=2 * rows * ff),
        name='expert_first' if first else 'expert_next')(*args)


def capacity_of(tok_rows, top_k, experts):
    return 8 * ((5 * tok_rows * top_k + 32 * experts - 1) // (32 * experts))


def positions(own_ref, owners):
    tokens = own_ref.shape[1]
    who = lax.broadcasted_iota(jnp.int32, (owners, tokens), 0)
    chosen = (own_ref[0:1, :] == who) | (own_ref[1:2, :] == who)
    before = lax.broadcasted_iota(jnp.int32, (tokens, tokens), 0) < lax.broadcasted_iota(jnp.int32, (tokens, tokens), 1)
    flags = jnp.where(chosen, 1.0, 0.0).astype(BF16)
    place = jnp.dot(flags, jnp.where(before, 1.0, 0.0).astype(BF16), preferred_element_type=F32)
    return jnp.where(chosen, place, -1.0)


def dispatch_kernel(owners, cap, own_ref, x_ref, dy_ref, after, xdy_ref, pos_v):
    step = pl.program_id(0)
    d = x_ref.shape[1]

    @pl.when(step == 0)
    def _():
        pos_v[...] = positions(own_ref, owners)

    place = pos_v[pl.ds(step, 1), :].astype(jnp.int32)
    hit = place == lax.broadcasted_iota(jnp.int32, (cap, place.shape[1]), 0)
    pick = jnp.where(hit, 1.0, 0.0).astype(BF16)
    xdy_ref[:, :d] = jnp.dot(pick, x_ref[...], preferred_element_type=F32).astype(BF16)
    xdy_ref[:, d:] = jnp.dot(pick, dy_ref[...], preferred_element_type=F32).astype(BF16)


def dispatch(own_t, x_in, dy_out, mb, owners, cap, after):
    _, tokens, d = x_in.shape
    part = pl.BlockSpec((None, tokens, d), lambda i: (mb, 0, 0))
    return pl.pallas_call(
        functools.partial(dispatch_kernel, owners, cap),
        grid=(owners,),
        in_specs=[pl.BlockSpec((None, 2, tokens), lambda i: (mb, 0, 0)), part, part, pl.BlockSpec(memory_space=pl.ANY)],
        out_specs=pl.BlockSpec((cap, 2 * d), lambda i: (i, 0)),
        out_shape=jax.ShapeDtypeStruct((owners * cap, 2 * d), BF16),
        scratch_shapes=[pltpu.VMEM((owners, tokens), F32)],
        compiler_params=pltpu.CompilerParams(vmem_limit_bytes=60 * 2**20),
        cost_estimate=pl.CostEstimate(flops=4 * owners * cap * tokens * d, bytes_accessed=8 * 2**20, transcendentals=0))(own_t, x_in, dy_out, after)


def gates_kernel(cap, here_sm, table_ref, gate_ref, cols_v):
    blocks, tokens = table_ref.shape[0], table_ref.shape[2]
    here = here_sm[0].astype(F32)
    first = jnp.concatenate([table_ref[k, 0:1, :] for k in range(blocks)], axis=0) == here
    second = jnp.concatenate([table_ref[k, 1:2, :] for k in range(blocks)], axis=0) == here
    before = lax.broadcasted_iota(jnp.int32, (tokens, tokens), 0) < lax.broadcasted_iota(jnp.int32, (tokens, tokens), 1)
    flags = jnp.where(first | second, 1.0, 0.0).astype(BF16)
    place = jnp.dot(flags, jnp.where(before, 1.0, 0.0).astype(BF16), preferred_element_type=F32)
    place = jnp.where(first | second, place, -1.0).astype(jnp.int32)
    iota = lax.broadcasted_iota(jnp.int32, (cap, tokens), 0)
    cols_v[...] = jnp.zeros_like(cols_v)
    for k in range(blocks):
        gate = jnp.where(first[k:k + 1, :], table_ref[k, 2:3, :], table_ref[k, 3:4, :])
        cols_v[:, k:k + 1] = jnp.sum(jnp.where(place[k:k + 1, :] == iota, gate, 0.0), axis=1, keepdims=True)
    gate_ref[...] = cols_v[...].T[:blocks, :]


def slot_gates(here, table, cap):
    blocks, _, _ = table.shape
    vm = pl.BlockSpec(memory_space=pltpu.VMEM)
    return pl.pallas_call(
        functools.partial(gates_kernel, cap),
        in_specs=[pl.BlockSpec(memory_space=pltpu.SMEM), vm],
        out_specs=vm,
        out_shape=jax.ShapeDtypeStruct((blocks, cap), F32),
        scratch_shapes=[pltpu.VMEM((cap, 128), F32)],
        cost_estimate=pl.CostEstimate(flops=10 * 2**30, bytes_accessed=2**20, transcendentals=0),
        name='slot_gates')(here, table)


def combine_kernel(owners, cap, n_sm, own_ref, back_ref, dg_ref, *rest):
    dx_ref, dgate_ref, rows_v = rest[-3:]
    tokens = own_ref.shape[1]
    d = back_ref.shape[1]
    pos = positions(own_ref, owners)
    dg_cols = dg_ref[...].T
    place_iota = lax.broadcasted_iota(jnp.int32, (cap, tokens), 0)
    row_iota = lax.broadcasted_iota(jnp.int32, (cap, d), 0)
    dgate = [jnp.zeros((1, tokens), F32), jnp.zeros((1, tokens), F32)]
    slot = [jnp.full((1, tokens), -1, jnp.int32), jnp.full((1, tokens), -1, jnp.int32)]
    for k in range(owners):
        place = pos[k:k + 1, :].astype(jnp.int32)
        got = jnp.sum(jnp.where(place == place_iota, dg_cols[:, k:k + 1], 0.0), axis=0, keepdims=True)
        kept = jnp.where(place < cap, place + k * cap, -1)
        for j in range(2):
            mine = own_ref[j:j + 1, :] == k
            dgate[j] = jnp.where(mine, got, dgate[j])
            slot[j] = jnp.where(mine, kept, slot[j])
        rows = back_ref[k * cap:(k + 1) * cap, :].astype(F32)
        rows_v[k * cap:(k + 1) * cap, :] = jnp.where(row_iota < n_sm[k], rows, 0.0).astype(BF16)
    dgate_ref[0:1, :] = dgate[0]
    dgate_ref[1:2, :] = dgate[1]
    slots = jnp.concatenate([s.astype(F32) for s in slot] + [jnp.zeros((6, tokens), F32)], axis=0).T.astype(jnp.int32)
    step = 256
    for lo in range(0, tokens, step):
        iota = lax.broadcasted_iota(jnp.int32, (step, owners * cap), 1)
        hit = (slots[lo:lo + step, 0:1] == iota) | (slots[lo:lo + step, 1:2] == iota)
        pick = jnp.where(hit, 1.0, 0.0).astype(BF16)
        dx_ref[lo:lo + step, :] = jnp.dot(pick, rows_v[...], preferred_element_type=F32).astype(BF16)


def combine(n_kept, own_t, back, dg_back, mb, cap, done):
    rows, d = back.shape
    owners = n_kept.shape[0]
    micro, _, tokens = own_t.shape
    vm = pl.BlockSpec(memory_space=pltpu.VMEM)
    whole = pl.BlockSpec(memory_space=pl.ANY)
    return pl.pallas_call(
        functools.partial(combine_kernel, owners, cap),
        grid=(1,),
        in_specs=[pl.BlockSpec(memory_space=pltpu.SMEM), pl.BlockSpec((None, 2, tokens), lambda i: (mb, 0, 0)), vm, vm] + [whole] * len(done),
        out_specs=[pl.BlockSpec((None, tokens, d), lambda i: (mb, 0, 0)), pl.BlockSpec((None, 2, tokens), lambda i: (mb, 0, 0))],
        out_shape=[jax.ShapeDtypeStruct((micro, tokens, d), BF16), jax.ShapeDtypeStruct((micro, 2, tokens), F32)],
        input_output_aliases={4: 0, 5: 1} if done else {},
        scratch_shapes=[pltpu.VMEM((rows, d), BF16)],
        compiler_params=pltpu.CompilerParams(vmem_limit_bytes=60 * 2**20),
        cost_estimate=pl.CostEstimate(flops=2 * rows * tokens * d, bytes_accessed=6 * 2**20, transcendentals=0))(n_kept, own_t, back, dg_back, *done)


def solution(mesh):
    side = round(mesh.shape['fsdp'] ** (1 / 3))
    cores = mesh.shape['ep']
    grid_mesh = Mesh(mesh.devices.reshape(side, side, side, cores), ('z', 'y', 'x', 'c'))
    tok_spec = P(None, ('z', 'y', 'x', 'c'), None)
    spec_edf = P('c', ('z', 'y', 'x'), None)
    spec_efd = P('c', None, ('z', 'y', 'x'))
    ring = ('x', 'c')

    def local_step(x_in, dy_out, expert_idx, gate_prob, w_one, w_two, w_three):
        micro_count, tok_rows, d_model = x_in.shape
        top_k = expert_idx.shape[2]
        local_experts, shard, ff = w_one.shape
        experts = local_experts * cores
        cap = capacity_of(tok_rows, top_k, experts)
        rows = experts * cap
        ids_t = jnp.transpose(expert_idx, (0, 2, 1))
        own_t = (ids_t % local_experts) * cores + ids_t // local_experts
        q_t = jnp.transpose(gate_prob, (0, 2, 1))
        here = lax.axis_index('x') * cores + lax.axis_index('c')
        table = lax.all_gather(jnp.concatenate([own_t.astype(F32), q_t], axis=1), ring, axis=1)
        table = table.reshape(micro_count * experts, 2 * top_k, tok_rows)
        n_here = jnp.sum((table[:, :top_k] == here.astype(F32)).astype(jnp.int32), axis=(1, 2))
        n_recv = ((jnp.minimum(n_here, cap) + UNIT - 1) // UNIT).reshape(micro_count, experts)
        picks = (own_t[:, :, :, None] == jnp.arange(experts, dtype=jnp.int32)).astype(jnp.int32)
        n_kept = jnp.minimum(jnp.sum(picks, axis=(1, 2)), cap)
        w_cat = jnp.concatenate([w_one, jnp.transpose(w_two, (0, 2, 1)), w_three], axis=2)
        x_id = lax.axis_index('x')
        dealt = [lax.dynamic_index_in_dim(w_cat, x_id, 0, keepdims=False)]
        for k in range(1, local_experts):
            piece = lax.dynamic_index_in_dim(w_cat, (x_id + k) % local_experts, 0, keepdims=False)
            dealt.append(lax.ppermute(piece, 'x', [(i, (i + k) % local_experts) for i in range(local_experts)]))
        slabs = []
        for j in range(local_experts):
            back = (x_id - j) % local_experts
            slab = dealt[0]
            for k in range(1, local_experts):
                slab = jnp.where(back == k, dealt[k], slab)
            slabs.append(slab)
        w_mine = jnp.concatenate(slabs, axis=0)
        w_full = lax.all_gather(w_mine, ('z', 'y'), axis=0, tiled=True)
        xdy = []
        for mb in range(micro_count):
            send = dispatch(own_t, x_in, dy_out, mb, experts, cap, table)
            xdy.append(lax.all_to_all(send.reshape(experts, cap, 2 * d_model), ring, 0, 0, tiled=True).reshape(rows, 2 * d_model))
        gate_rows = slot_gates(here.reshape(1), table, cap).reshape(micro_count, experts, cap)
        dx_back = []
        dg_rows = []
        grad_sum = None
        for mb in range(micro_count):
            dx_rows, dg, grad_sum = expert_pass(n_recv[mb], xdy[mb], gate_rows[mb], w_full, grad_sum)
            dx_back.append(lax.all_to_all(dx_rows.reshape(experts, cap, d_model), ring, 0, 0, tiled=True).reshape(rows, d_model))
            dg_rows.append(dg)
        dw_mine = lax.psum_scatter(grad_sum, ('z', 'y'), scatter_dimension=0, tiled=True)
        dg_back = lax.all_to_all(jnp.stack(dg_rows, axis=1), ring, 0, 0, tiled=True)
        done = []
        for mb in range(micro_count):
            done = combine(n_kept[mb], own_t, dx_back[mb], dg_back[:, mb], mb, cap, done)
        dx_in, d_gate = done[0], jnp.transpose(done[1], (0, 2, 1))
        dw_all = lax.all_to_all(dw_mine.reshape(local_experts, shard, 3 * ff), 'x', 0, 0, tiled=True)
        dw_one, dw_two, dw_three = dw_all[:, :, :ff], jnp.transpose(dw_all[:, :, ff:2 * ff], (0, 2, 1)), dw_all[:, :, 2 * ff:]
        return dx_in, d_gate, dw_one, dw_two, dw_three

    return jax.shard_map(local_step, mesh=grid_mesh, in_specs=(tok_spec, tok_spec, tok_spec, tok_spec, spec_edf, spec_efd, spec_edf), out_specs=(tok_spec, tok_spec, spec_edf, spec_efd, spec_edf), check_vma=False)
```

```python
import functools

import jax
import jax.numpy as jnp
from jax import lax
from jax.experimental import pallas as pl
from jax.experimental.pallas import tpu as pltpu
from jax.sharding import Mesh, PartitionSpec as P


F32 = jnp.float32
BF16 = jnp.bfloat16
UNIT = 16
COL_TILE = 256
NT_DIMS = (((1,),(1,)),((),()))


def row_pieces(n_sm, cap, emit):
    off = jnp.int32(0)
    for s in range(n_sm.shape[0]):
        n = n_sm[s]
        for k in range(cap // 64):
            @pl.when((k + 1) * 4 <= n)
            def _(k=k, s=s, off=off):
                emit(s * cap + k * 64, off * UNIT + k * 64, 64)
        base = (n // 4) * 4

        @pl.when((n // 2) % 2 == 1)
        def _(s=s, off=off, base=base):
            emit(s * cap + base * UNIT, (off + base) * UNIT, 32)

        tail = (n // 2) * 2

        @pl.when(n % 2 == 1)
        def _(s=s, off=off, tail=tail):
            emit(s * cap + tail * UNIT, (off + tail) * UNIT, 16)

        off = off + n
    return off


def expert_kernel(ff, cap, first, n_sm, xdy_hbm, q_ref, w_hbm, *rest):
    if first:
        dx_hbm, dg_ref, gw_hbm, xdy_v, q_v, dg_v, dx_v, w_v, gw_v, xt_v, gt_v, sems = rest
        gin_hbm = gin_v = None
    else:
        gin_hbm, dx_hbm, dg_ref, gw_hbm, xdy_v, q_v, dg_v, dx_v, w_v, gw_v, xt_v, gt_v, gin_v, sems = rest
    d = w_hbm.shape[0]
    n_src = n_sm.shape[0]

    def m8(v, n=UNIT):
        return v if isinstance(v, int) else pl.multiple_of(v, n)

    def fetch(slot, packed, size):
        return pltpu.make_async_copy(xdy_hbm.at[pl.ds(m8(slot), size)], xdy_v.at[pl.ds(m8(packed), size)], sems.at[0])

    units = row_pieces(n_sm, cap, lambda *a: fetch(*a).start())
    parts = [pltpu.make_async_copy(w_hbm.at[:, pl.ds(k * ff, ff)], w_v.at[:, pl.ds(k * ff, ff)], sems.at[1 + k]) for k in range(3)]
    for p in parts:
        p.start()
    if not first:
        gin = pltpu.make_async_copy(gin_hbm, gin_v, sems.at[4])
        gin.start()
    gw_v[...] = jnp.zeros_like(gw_v)
    q_cols = q_ref[...].T
    off = jnp.int32(0)
    for s in range(n_src):
        q_v[pl.ds(pl.multiple_of(off * UNIT, UNIT), cap), :] = q_cols[:, s:s + 1]
        off = off + n_sm[s]
    q_v[pl.ds(pl.multiple_of(off * UNIT, UNIT), 512), :] = jnp.zeros((512, 1), F32)

    def clear(i, c):
        xdy_v[pl.ds(pl.multiple_of(i * UNIT, UNIT), UNIT), :] = jnp.zeros((UNIT, 2 * d), BF16)
        return c

    lax.fori_loop(units, ((units + 15) // 16) * 16, clear, 0)
    row_pieces(n_sm, cap, lambda *a: fetch(*a).wait())
    for p in parts:
        p.wait()

    dot = functools.partial(jnp.dot, preferred_element_type=F32)
    dot_nt = lambda a, b: lax.dot_general(a, b, NT_DIMS, preferred_element_type=F32)

    def tile(lo_row, rt):
        rows = pl.ds(pl.multiple_of(lo_row, 256), rt)
        x = xdy_v[rows, :d]
        dy = xdy_v[rows, d:]
        g = (q_v[rows, :] * dy.astype(F32)).astype(BF16)
        xt_v[:, :rt] = x.T
        gt_v[:, :rt] = g.T
        y = None
        dx = None
        for lo in range(0, ff, COL_TILE):
            one, two, three = (pl.ds(k * ff + lo, COL_TILE) for k in range(3))
            h_one = dot(x, w_v[:, one])
            h_three = dot(x, w_v[:, three])
            d_act = dot(g, w_v[:, two])
            sigma = jax.nn.sigmoid(h_one)
            silu = h_one * sigma
            act = (silu * h_three).astype(BF16)
            dh_three = (d_act * silu).astype(BF16)
            dh_one = (d_act * h_three * sigma * (1.0 + h_one * (1.0 - sigma))).astype(BF16)
            y_part = dot_nt(act, w_v[:, two])
            dx_part = dot_nt(dh_one, w_v[:, one]) + dot_nt(dh_three, w_v[:, three])
            y = y_part if y is None else y + y_part
            dx = dx_part if dx is None else dx + dx_part
            gw_v[:, one] += dot(xt_v[:, :rt], dh_one)
            gw_v[:, three] += dot(xt_v[:, :rt], dh_three)
            gw_v[:, two] += dot(gt_v[:, :rt], act)
        dg_v[rows, :] = jnp.sum(dy.astype(F32) * y, axis=1, keepdims=True)
        dx_v[rows, :] = dx.astype(BF16)

    total = units * UNIT
    full = (total + 255) // 512

    def big(i, c):
        tile(i * 512, 512)
        return c

    lax.fori_loop(0, full, big, 0)

    @pl.when(full * 512 < total)
    def _():
        tile(full * 512, 256)

    if not first:
        gin.wait()
    outs = []
    for k in range(3):
        cols = pl.ds(k * ff, ff)
        if not first:
            gw_v[:, cols] += gin_v[:, cols]
        o = pltpu.make_async_copy(gw_v.at[:, cols], gw_hbm.at[:, cols], sems.at[1 + k])
        o.start()
        outs.append(o)

    def put(slot, packed, size):
        return pltpu.make_async_copy(dx_v.at[pl.ds(m8(packed), size)], dx_hbm.at[pl.ds(m8(slot), size)], sems.at[0])

    row_pieces(n_sm, cap, lambda *a: put(*a).start())
    off = jnp.int32(0)
    cols = []
    for s in range(n_src):
        cols.append(dg_v[pl.ds(pl.multiple_of(off * UNIT, UNIT), cap), :])
        off = off + n_sm[s]
    dg_ref[...] = jnp.concatenate(cols, axis=1).T
    row_pieces(n_sm, cap, lambda *a: put(*a).wait())
    for o in outs:
        o.wait()


def expert_pass(n_units, xdy, gates, w_full, grad_in):
    rows, d2 = xdy.shape
    d = d2 // 2
    ff = w_full.shape[1] // 3
    cap = gates.shape[1]
    first = grad_in is None
    whole = pl.BlockSpec(memory_space=pl.ANY)
    vm = pl.BlockSpec(memory_space=pltpu.VMEM)
    args = [n_units, xdy, gates, w_full] + ([] if first else [grad_in])
    in_specs = [pl.BlockSpec(memory_space=pltpu.SMEM), whole, vm, whole] + ([] if first else [whole])
    pad = rows + 512
    scratch = [
        pltpu.VMEM((rows, d2), BF16), pltpu.VMEM((pad, 1), F32), pltpu.VMEM((pad, 1), F32), pltpu.VMEM((rows, d), BF16),
        pltpu.VMEM((d, 3 * ff), BF16), pltpu.VMEM((d, 3 * ff), F32), pltpu.VMEM((d, 512), BF16), pltpu.VMEM((d, 512), BF16)]
    if not first:
        scratch.append(pltpu.VMEM((d, 3 * ff), F32))
    scratch.append(pltpu.SemaphoreType.DMA((5,)))
    return pl.pallas_call(
        functools.partial(expert_kernel, ff, cap, first),
        in_specs=in_specs, out_specs=[whole, vm, whole],
        out_shape=[jax.ShapeDtypeStruct((rows, d), BF16), jax.ShapeDtypeStruct(gates.shape, F32), jax.ShapeDtypeStruct((d, 3 * ff), F32)],
        scratch_shapes=scratch,
        compiler_params=pltpu.CompilerParams(vmem_limit_bytes=60 * 2**20),
        cost_estimate=pl.CostEstimate(flops=18 * rows * d * ff, bytes_accessed=40 * 2**20, transcendentals=2 * rows * ff),
        name='expert_first' if first else 'expert_next')(*args)


def capacity_of(tok_rows, top_k, experts):
    return 8 * ((5 * tok_rows * top_k + 32 * experts - 1) // (32 * experts))


def positions(own_ref, owners):
    tokens = own_ref.shape[1]
    who = lax.broadcasted_iota(jnp.int32, (owners, tokens), 0)
    chosen = (own_ref[0:1, :] == who) | (own_ref[1:2, :] == who)
    before = lax.broadcasted_iota(jnp.int32, (tokens, tokens), 0) < lax.broadcasted_iota(jnp.int32, (tokens, tokens), 1)
    flags = jnp.where(chosen, 1.0, 0.0).astype(BF16)
    place = jnp.dot(flags, jnp.where(before, 1.0, 0.0).astype(BF16), preferred_element_type=F32)
    return jnp.where(chosen, place, -1.0)


def dispatch_kernel(owners, cap, own_ref, x_ref, dy_ref, xdy_ref, pos_v):
    step = pl.program_id(0)
    d = x_ref.shape[1]

    @pl.when(step == 0)
    def _():
        pos_v[...] = positions(own_ref, owners)

    place = pos_v[pl.ds(step, 1), :].astype(jnp.int32)
    hit = place == lax.broadcasted_iota(jnp.int32, (cap, place.shape[1]), 0)
    pick = jnp.where(hit, 1.0, 0.0).astype(BF16)
    xdy_ref[:, :d] = jnp.dot(pick, x_ref[...], preferred_element_type=F32).astype(BF16)
    xdy_ref[:, d:] = jnp.dot(pick, dy_ref[...], preferred_element_type=F32).astype(BF16)


def dispatch(own_t, x_in, dy_out, mb, owners, cap):
    _, tokens, d = x_in.shape
    part = pl.BlockSpec((None, tokens, d), lambda i: (mb, 0, 0))
    return pl.pallas_call(
        functools.partial(dispatch_kernel, owners, cap),
        grid=(owners,),
        in_specs=[pl.BlockSpec((None, 2, tokens), lambda i: (mb, 0, 0)), part, part],
        out_specs=pl.BlockSpec((cap, 2 * d), lambda i: (i, 0)),
        out_shape=jax.ShapeDtypeStruct((owners * cap, 2 * d), BF16),
        scratch_shapes=[pltpu.VMEM((owners, tokens), F32)],
        compiler_params=pltpu.CompilerParams(vmem_limit_bytes=60 * 2**20),
        cost_estimate=pl.CostEstimate(flops=4 * owners * cap * tokens * d, bytes_accessed=8 * 2**20, transcendentals=0))(own_t, x_in, dy_out)


def gates_kernel(cap, here_sm, table_ref, gate_ref, cols_v):
    blocks, tokens = table_ref.shape[0], table_ref.shape[2]
    here = here_sm[0].astype(F32)
    first = jnp.concatenate([table_ref[k, 0:1, :] for k in range(blocks)], axis=0) == here
    second = jnp.concatenate([table_ref[k, 1:2, :] for k in range(blocks)], axis=0) == here
    before = lax.broadcasted_iota(jnp.int32, (tokens, tokens), 0) < lax.broadcasted_iota(jnp.int32, (tokens, tokens), 1)
    flags = jnp.where(first | second, 1.0, 0.0).astype(BF16)
    place = jnp.dot(flags, jnp.where(before, 1.0, 0.0).astype(BF16), preferred_element_type=F32)
    place = jnp.where(first | second, place, -1.0).astype(jnp.int32)
    iota = lax.broadcasted_iota(jnp.int32, (cap, tokens), 0)
    cols_v[...] = jnp.zeros_like(cols_v)
    for k in range(blocks):
        gate = jnp.where(first[k:k + 1, :], table_ref[k, 2:3, :], table_ref[k, 3:4, :])
        cols_v[:, k:k + 1] = jnp.sum(jnp.where(place[k:k + 1, :] == iota, gate, 0.0), axis=1, keepdims=True)
    gate_ref[...] = cols_v[...].T[:blocks, :]


def slot_gates(here, table, cap):
    blocks, _, _ = table.shape
    vm = pl.BlockSpec(memory_space=pltpu.VMEM)
    return pl.pallas_call(
        functools.partial(gates_kernel, cap),
        in_specs=[pl.BlockSpec(memory_space=pltpu.SMEM), vm],
        out_specs=vm,
        out_shape=jax.ShapeDtypeStruct((blocks, cap), F32),
        scratch_shapes=[pltpu.VMEM((cap, 128), F32)],
        cost_estimate=pl.CostEstimate(flops=10 * 2**30, bytes_accessed=2**20, transcendentals=0),
        name='slot_gates')(here, table)


def combine_kernel(owners, cap, n_sm, own_ref, back_ref, dg_ref, *rest):
    dx_ref, dgate_ref, rows_v = rest[-3:]
    tokens = own_ref.shape[1]
    d = back_ref.shape[1]
    pos = positions(own_ref, owners)
    dg_cols = dg_ref[...].T
    place_iota = lax.broadcasted_iota(jnp.int32, (cap, tokens), 0)
    row_iota = lax.broadcasted_iota(jnp.int32, (cap, d), 0)
    dgate = [jnp.zeros((1, tokens), F32), jnp.zeros((1, tokens), F32)]
    slot = [jnp.full((1, tokens), -1, jnp.int32), jnp.full((1, tokens), -1, jnp.int32)]
    for k in range(owners):
        place = pos[k:k + 1, :].astype(jnp.int32)
        got = jnp.sum(jnp.where(place == place_iota, dg_cols[:, k:k + 1], 0.0), axis=0, keepdims=True)
        kept = jnp.where(place < cap, place + k * cap, -1)
        for j in range(2):
            mine = own_ref[j:j + 1, :] == k
            dgate[j] = jnp.where(mine, got, dgate[j])
            slot[j] = jnp.where(mine, kept, slot[j])
        rows = back_ref[k * cap:(k + 1) * cap, :].astype(F32)
        rows_v[k * cap:(k + 1) * cap, :] = jnp.where(row_iota < n_sm[k], rows, 0.0).astype(BF16)
    dgate_ref[0:1, :] = dgate[0]
    dgate_ref[1:2, :] = dgate[1]
    slots = jnp.concatenate([s.astype(F32) for s in slot] + [jnp.zeros((6, tokens), F32)], axis=0).T.astype(jnp.int32)
    step = 256
    for lo in range(0, tokens, step):
        iota = lax.broadcasted_iota(jnp.int32, (step, owners * cap), 1)
        hit = (slots[lo:lo + step, 0:1] == iota) | (slots[lo:lo + step, 1:2] == iota)
        pick = jnp.where(hit, 1.0, 0.0).astype(BF16)
        dx_ref[lo:lo + step, :] = jnp.dot(pick, rows_v[...], preferred_element_type=F32).astype(BF16)


def combine(n_kept, own_t, back, dg_back, mb, cap, done):
    rows, d = back.shape
    owners = n_kept.shape[0]
    micro, _, tokens = own_t.shape
    vm = pl.BlockSpec(memory_space=pltpu.VMEM)
    whole = pl.BlockSpec(memory_space=pl.ANY)
    return pl.pallas_call(
        functools.partial(combine_kernel, owners, cap),
        grid=(1,),
        in_specs=[pl.BlockSpec(memory_space=pltpu.SMEM), pl.BlockSpec((None, 2, tokens), lambda i: (mb, 0, 0)), vm, vm] + [whole] * len(done),
        out_specs=[pl.BlockSpec((None, tokens, d), lambda i: (mb, 0, 0)), pl.BlockSpec((None, 2, tokens), lambda i: (mb, 0, 0))],
        out_shape=[jax.ShapeDtypeStruct((micro, tokens, d), BF16), jax.ShapeDtypeStruct((micro, 2, tokens), F32)],
        input_output_aliases={4: 0, 5: 1} if done else {},
        scratch_shapes=[pltpu.VMEM((rows, d), BF16)],
        compiler_params=pltpu.CompilerParams(vmem_limit_bytes=60 * 2**20),
        cost_estimate=pl.CostEstimate(flops=2 * rows * tokens * d, bytes_accessed=6 * 2**20, transcendentals=0))(n_kept, own_t, back, dg_back, *done)


def solution(mesh):
    side = round(mesh.shape['fsdp'] ** (1 / 3))
    cores = mesh.shape['ep']
    grid_mesh = Mesh(mesh.devices.reshape(side, side, side, cores), ('z', 'y', 'x', 'c'))
    tok_spec = P(None, ('z', 'y', 'x', 'c'), None)
    spec_edf = P('c', ('z', 'y', 'x'), None)
    spec_efd = P('c', None, ('z', 'y', 'x'))
    ring = ('x', 'c')

    def local_step(x_in, dy_out, expert_idx, gate_prob, w_one, w_two, w_three):
        micro_count, tok_rows, d_model = x_in.shape
        top_k = expert_idx.shape[2]
        local_experts, shard, ff = w_one.shape
        experts = local_experts * cores
        cap = capacity_of(tok_rows, top_k, experts)
        rows = experts * cap
        ids_t = jnp.transpose(expert_idx, (0, 2, 1))
        own_t = (ids_t % local_experts) * cores + ids_t // local_experts
        q_t = jnp.transpose(gate_prob, (0, 2, 1))
        here = lax.axis_index('x') * cores + lax.axis_index('c')
        mine = jnp.concatenate([own_t.astype(F32), q_t], axis=1)
        tables = [mine]
        for k in range(1, experts):
            tables.append(lax.ppermute(mine, ring, [(i, (i + k) % experts) for i in range(experts)]))
        table = jnp.stack(tables, axis=1).reshape(micro_count * experts, 2 * top_k, tok_rows)
        source = jnp.arange(experts, dtype=jnp.int32)
        is_from = (here - source[:, None]) % experts == source[None, :]
        n_here = jnp.sum((table[:, :top_k] == here.astype(F32)).astype(jnp.int32), axis=(1, 2)).reshape(micro_count, 1, experts)
        n_here = jnp.sum(jnp.where(is_from, n_here, 0), axis=2)
        n_recv = (jnp.minimum(n_here, cap) + UNIT - 1) // UNIT
        picks = (own_t[:, :, :, None] == jnp.arange(experts, dtype=jnp.int32)).astype(jnp.int32)
        n_kept = jnp.minimum(jnp.sum(picks, axis=(1, 2)), cap)
        w_cat = jnp.concatenate([w_one, jnp.transpose(w_two, (0, 2, 1)), w_three], axis=2)
        x_id = lax.axis_index('x')

        def deal(slabs):
            dealt = [lax.dynamic_index_in_dim(slabs, x_id, 0, keepdims=False)]
            for k in range(1, local_experts):
                piece = lax.dynamic_index_in_dim(slabs, (x_id + k) % local_experts, 0, keepdims=False)
                dealt.append(lax.ppermute(piece, 'x', [(i, (i + k) % local_experts) for i in range(local_experts)]))
            result = []
            for j in range(local_experts):
                back = (x_id - j) % local_experts
                slab = dealt[0]
                for k in range(1, local_experts):
                    slab = jnp.where(back == k, dealt[k], slab)
                result.append(slab)
            return result

        w_mine = jnp.concatenate(deal(w_cat), axis=0)
        w_full = lax.all_gather(w_mine, ('z', 'y'), axis=0, tiled=True)
        xdy = []
        for mb in range(micro_count):
            send = dispatch(own_t, x_in, dy_out, mb, experts, cap)
            xdy.append(lax.all_to_all(send.reshape(experts, cap, 2 * d_model), ring, 0, 0, tiled=True).reshape(rows, 2 * d_model))
        gate_rows = slot_gates(here.reshape(1), table, cap).reshape(micro_count, 1, experts, cap)
        gate_rows = jnp.sum(jnp.where(is_from[:, :, None], gate_rows, 0.0), axis=2)
        dx_back = []
        dg_rows = []
        grad_sum = None
        for mb in range(micro_count):
            dx_rows, dg, grad_sum = expert_pass(n_recv[mb], xdy[mb], gate_rows[mb], w_full, grad_sum)
            dx_back.append(lax.all_to_all(dx_rows.reshape(experts, cap, d_model), ring, 0, 0, tiled=True).reshape(rows, d_model))
            dg_rows.append(dg)
        dw_mine = lax.psum_scatter(grad_sum, ('z', 'y'), scatter_dimension=0, tiled=True)
        dg_back = lax.all_to_all(jnp.stack(dg_rows, axis=1), ring, 0, 0, tiled=True)
        done = []
        for mb in range(micro_count):
            done = combine(n_kept[mb], own_t, dx_back[mb], dg_back[:, mb], mb, cap, done)
        dx_in, d_gate = done[0], jnp.transpose(done[1], (0, 2, 1))
        dw_all = jnp.stack(deal(dw_mine.reshape(local_experts, shard, 3 * ff)))
        dw_one, dw_two, dw_three = dw_all[:, :, :ff], jnp.transpose(dw_all[:, :, ff:2 * ff], (0, 2, 1)), dw_all[:, :, 2 * ff:]
        return dx_in, d_gate, dw_one, dw_two, dw_three

    return jax.shard_map(local_step, mesh=grid_mesh, in_specs=(tok_spec, tok_spec, tok_spec, tok_spec, spec_edf, spec_efd, spec_edf), out_specs=(tok_spec, tok_spec, spec_edf, spec_efd, spec_edf), check_vma=False)
```

```python
import functools

import jax
import jax.numpy as jnp
from jax import lax
from jax.experimental import pallas as pl
from jax.experimental.pallas import tpu as pltpu
from jax.sharding import Mesh, PartitionSpec as P


F32 = jnp.float32
BF16 = jnp.bfloat16
UNIT = 16
COL_TILE = 256
NT_DIMS = (((1,),(1,)),((),()))


def row_pieces(n_sm, cap, emit):
    off = jnp.int32(0)
    for s in range(n_sm.shape[0]):
        n = n_sm[s]
        for k in range(cap // 64):
            @pl.when((k + 1) * 4 <= n)
            def _(k=k, s=s, off=off):
                emit(s * cap + k * 64, off * UNIT + k * 64, 64)
        base = (n // 4) * 4

        @pl.when((n // 2) % 2 == 1)
        def _(s=s, off=off, base=base):
            emit(s * cap + base * UNIT, (off + base) * UNIT, 32)

        tail = (n // 2) * 2

        @pl.when(n % 2 == 1)
        def _(s=s, off=off, tail=tail):
            emit(s * cap + tail * UNIT, (off + tail) * UNIT, 16)

        off = off + n
    return off


def expert_kernel(ff, cap, first, n_sm, xdy_hbm, q_ref, w_hbm, *rest):
    if first:
        dx_hbm, dg_ref, gw_hbm, xdy_v, q_v, dg_v, dx_v, w_v, gw_v, xt_v, gt_v, sems = rest
        gin_hbm = gin_v = None
    else:
        gin_hbm, dx_hbm, dg_ref, gw_hbm, xdy_v, q_v, dg_v, dx_v, w_v, gw_v, xt_v, gt_v, gin_v, sems = rest
    d = w_hbm.shape[0]
    n_src = n_sm.shape[0]

    def m8(v, n=UNIT):
        return v if isinstance(v, int) else pl.multiple_of(v, n)

    def fetch(slot, packed, size):
        return pltpu.make_async_copy(xdy_hbm.at[pl.ds(m8(slot), size)], xdy_v.at[pl.ds(m8(packed), size)], sems.at[0])

    units = row_pieces(n_sm, cap, lambda *a: fetch(*a).start())
    parts = [pltpu.make_async_copy(w_hbm.at[:, pl.ds(k * ff, ff)], w_v.at[:, pl.ds(k * ff, ff)], sems.at[1 + k]) for k in range(3)]
    for p in parts:
        p.start()
    if not first:
        gin = pltpu.make_async_copy(gin_hbm, gin_v, sems.at[4])
        gin.start()
    gw_v[...] = jnp.zeros_like(gw_v)
    q_cols = q_ref[...].T
    off = jnp.int32(0)
    for s in range(n_src):
        q_v[pl.ds(pl.multiple_of(off * UNIT, UNIT), cap), :] = q_cols[:, s:s + 1]
        off = off + n_sm[s]
    q_v[pl.ds(pl.multiple_of(off * UNIT, UNIT), 512), :] = jnp.zeros((512, 1), F32)

    def clear(i, c):
        xdy_v[pl.ds(pl.multiple_of(i * UNIT, UNIT), UNIT), :] = jnp.zeros((UNIT, 2 * d), BF16)
        return c

    lax.fori_loop(units, ((units + 31) // 32) * 32, clear, 0)
    row_pieces(n_sm, cap, lambda *a: fetch(*a).wait())
    for p in parts:
        p.wait()

    dot = functools.partial(jnp.dot, preferred_element_type=F32)
    dot_nt = lambda a, b: lax.dot_general(a, b, NT_DIMS, preferred_element_type=F32)

    def tile(lo_row, rt):
        rows = pl.ds(pl.multiple_of(lo_row, 256), rt)
        x = xdy_v[rows, :d]
        dy = xdy_v[rows, d:]
        g = (q_v[rows, :] * dy.astype(F32)).astype(BF16)
        xt_v[:, :rt] = x.T
        gt_v[:, :rt] = g.T
        y = None
        dx = None
        for lo in range(0, ff, COL_TILE):
            one, two, three = (pl.ds(k * ff + lo, COL_TILE) for k in range(3))
            h_one = dot(x, w_v[:, one])
            h_three = dot(x, w_v[:, three])
            d_act = dot(g, w_v[:, two])
            sigma = jax.nn.sigmoid(h_one)
            silu = h_one * sigma
            act = (silu * h_three).astype(BF16)
            dh_three = (d_act * silu).astype(BF16)
            dh_one = (d_act * h_three * sigma * (1.0 + h_one * (1.0 - sigma))).astype(BF16)
            y_part = dot_nt(act, w_v[:, two])
            dx_part = dot_nt(dh_one, w_v[:, one]) + dot_nt(dh_three, w_v[:, three])
            y = y_part if y is None else y + y_part
            dx = dx_part if dx is None else dx + dx_part
            gw_v[:, one] += dot(xt_v[:, :rt], dh_one)
            gw_v[:, three] += dot(xt_v[:, :rt], dh_three)
            gw_v[:, two] += dot(gt_v[:, :rt], act)
        dg_v[rows, :] = jnp.sum(dy.astype(F32) * y, axis=1, keepdims=True)
        dx_v[rows, :] = dx.astype(BF16)

    total = units * UNIT
    full = (total + 511) // 512

    def big(i, c):
        tile(i * 512, 512)
        return c

    lax.fori_loop(0, full, big, 0)

    if not first:
        gin.wait()
    outs = []
    for k in range(3):
        cols = pl.ds(k * ff, ff)
        if not first:
            gw_v[:, cols] += gin_v[:, cols]
        o = pltpu.make_async_copy(gw_v.at[:, cols], gw_hbm.at[:, cols], sems.at[1 + k])
        o.start()
        outs.append(o)

    def put(slot, packed, size):
        return pltpu.make_async_copy(dx_v.at[pl.ds(m8(packed), size)], dx_hbm.at[pl.ds(m8(slot), size)], sems.at[0])

    row_pieces(n_sm, cap, lambda *a: put(*a).start())
    off = jnp.int32(0)
    cols = []
    for s in range(n_src):
        cols.append(dg_v[pl.ds(pl.multiple_of(off * UNIT, UNIT), cap), :])
        off = off + n_sm[s]
    dg_ref[...] = jnp.concatenate(cols, axis=1).T
    row_pieces(n_sm, cap, lambda *a: put(*a).wait())
    for o in outs:
        o.wait()


def expert_pass(n_units, xdy, gates, w_full, grad_in):
    rows, d2 = xdy.shape
    d = d2 // 2
    ff = w_full.shape[1] // 3
    cap = gates.shape[1]
    first = grad_in is None
    whole = pl.BlockSpec(memory_space=pl.ANY)
    vm = pl.BlockSpec(memory_space=pltpu.VMEM)
    args = [n_units, xdy, gates, w_full] + ([] if first else [grad_in])
    in_specs = [pl.BlockSpec(memory_space=pltpu.SMEM), whole, vm, whole] + ([] if first else [whole])
    pad = rows + 512
    scratch = [
        pltpu.VMEM((rows, d2), BF16), pltpu.VMEM((pad, 1), F32), pltpu.VMEM((pad, 1), F32), pltpu.VMEM((rows, d), BF16),
        pltpu.VMEM((d, 3 * ff), BF16), pltpu.VMEM((d, 3 * ff), F32), pltpu.VMEM((d, 512), BF16), pltpu.VMEM((d, 512), BF16)]
    if not first:
        scratch.append(pltpu.VMEM((d, 3 * ff), F32))
    scratch.append(pltpu.SemaphoreType.DMA((5,)))
    return pl.pallas_call(
        functools.partial(expert_kernel, ff, cap, first),
        in_specs=in_specs, out_specs=[whole, vm, whole],
        out_shape=[jax.ShapeDtypeStruct((rows, d), BF16), jax.ShapeDtypeStruct(gates.shape, F32), jax.ShapeDtypeStruct((d, 3 * ff), F32)],
        scratch_shapes=scratch,
        compiler_params=pltpu.CompilerParams(vmem_limit_bytes=60 * 2**20),
        cost_estimate=pl.CostEstimate(flops=18 * rows * d * ff, bytes_accessed=40 * 2**20, transcendentals=2 * rows * ff),
        name='expert_first' if first else 'expert_next')(*args)


def capacity_of(tok_rows, top_k, experts):
    return 8 * ((5 * tok_rows * top_k + 32 * experts - 1) // (32 * experts))


def positions(own_ref, owners):
    tokens = own_ref.shape[1]
    who = lax.broadcasted_iota(jnp.int32, (owners, tokens), 0)
    chosen = (own_ref[0:1, :] == who) | (own_ref[1:2, :] == who)
    before = lax.broadcasted_iota(jnp.int32, (tokens, tokens), 0) < lax.broadcasted_iota(jnp.int32, (tokens, tokens), 1)
    flags = jnp.where(chosen, 1.0, 0.0).astype(BF16)
    place = jnp.dot(flags, jnp.where(before, 1.0, 0.0).astype(BF16), preferred_element_type=F32)
    return jnp.where(chosen, place, -1.0)


def dispatch_kernel(owners, cap, own_ref, x_ref, dy_ref, xdy_ref, pos_v):
    step = pl.program_id(0)
    d = x_ref.shape[1]

    @pl.when(step == 0)
    def _():
        pos_v[...] = positions(own_ref, owners)

    place = pos_v[pl.ds(step, 1), :].astype(jnp.int32)
    hit = place == lax.broadcasted_iota(jnp.int32, (cap, place.shape[1]), 0)
    pick = jnp.where(hit, 1.0, 0.0).astype(BF16)
    xdy_ref[:, :d] = jnp.dot(pick, x_ref[...], preferred_element_type=F32).astype(BF16)
    xdy_ref[:, d:] = jnp.dot(pick, dy_ref[...], preferred_element_type=F32).astype(BF16)


def dispatch(own_t, x_in, dy_out, mb, owners, cap):
    _, tokens, d = x_in.shape
    part = pl.BlockSpec((None, tokens, d), lambda i: (mb, 0, 0))
    return pl.pallas_call(
        functools.partial(dispatch_kernel, owners, cap),
        grid=(owners,),
        in_specs=[pl.BlockSpec((None, 2, tokens), lambda i: (mb, 0, 0)), part, part],
        out_specs=pl.BlockSpec((cap, 2 * d), lambda i: (i, 0)),
        out_shape=jax.ShapeDtypeStruct((owners * cap, 2 * d), BF16),
        scratch_shapes=[pltpu.VMEM((owners, tokens), F32)],
        compiler_params=pltpu.CompilerParams(vmem_limit_bytes=60 * 2**20),
        cost_estimate=pl.CostEstimate(flops=4 * owners * cap * tokens * d, bytes_accessed=8 * 2**20, transcendentals=0))(own_t, x_in, dy_out)


def gates_kernel(cap, here_sm, table_ref, gate_ref, cols_v, place_v, gate_v):
    blocks, tokens = table_ref.shape[0], table_ref.shape[2]
    here = here_sm[0].astype(F32)
    row = lambda j: jnp.concatenate([table_ref[k, j:j + 1, :] for k in range(blocks)], axis=0)
    first = row(0) == here
    chosen = first | (row(1) == here)
    before = lax.broadcasted_iota(jnp.int32, (tokens, tokens), 0) < lax.broadcasted_iota(jnp.int32, (tokens, tokens), 1)
    flags = jnp.where(chosen, 1.0, 0.0).astype(BF16)
    place = jnp.dot(flags, jnp.where(before, 1.0, 0.0).astype(BF16), preferred_element_type=F32)
    place_v[...] = jnp.where(chosen, place, -1.0).astype(jnp.int32)
    gate_v[...] = jnp.where(first, row(2), row(3))
    cols_v[...] = jnp.zeros_like(cols_v)

    def one(k, c):
        hit = place_v[pl.ds(k, 1), :] == lax.broadcasted_iota(jnp.int32, (cap, tokens), 0)
        column = jnp.sum(jnp.where(hit, gate_v[pl.ds(k, 1), :], 0.0), axis=1, keepdims=True)
        cols_v[...] += jnp.where(lax.broadcasted_iota(jnp.int32, cols_v.shape, 1) == k, column, 0.0)
        return c

    lax.fori_loop(0, blocks, one, 0)
    gate_ref[...] = cols_v[...].T[:blocks, :]


def slot_gates(here, table, cap):
    blocks, _, tokens = table.shape
    vm = pl.BlockSpec(memory_space=pltpu.VMEM)
    return pl.pallas_call(
        functools.partial(gates_kernel, cap),
        in_specs=[pl.BlockSpec(memory_space=pltpu.SMEM), vm],
        out_specs=vm,
        out_shape=jax.ShapeDtypeStruct((blocks, cap), F32),
        scratch_shapes=[pltpu.VMEM((cap, 128), F32), pltpu.VMEM((blocks, tokens), jnp.int32), pltpu.VMEM((blocks, tokens), F32)],
        cost_estimate=pl.CostEstimate(flops=10 * 2**30, bytes_accessed=2**20, transcendentals=0),
        name='slot_gates')(here, table)


def combine_kernel(owners, cap, n_sm, own_ref, dg_ref, *rest):
    backs, (dx_ref, dgate_ref, rows_v, slots_v, pos_v, sem) = rest[:-6], rest[-6:]
    mb = pl.program_id(0)
    for k, back in enumerate(backs):
        @pl.when(mb == k)
        def _(back=back):
            copy = pltpu.make_async_copy(back, rows_v, sem)
            copy.start()
            copy.wait()
    tokens = own_ref.shape[1]
    d = rows_v.shape[1]
    pos_v[...] = positions(own_ref, owners)
    dg_cols = dg_ref[...].T
    place_iota = lax.broadcasted_iota(jnp.int32, (cap, tokens), 0)
    row_iota = lax.broadcasted_iota(jnp.int32, (cap, d), 0)

    def one(k, c):
        dgate, slot = list(c[:2]), list(c[2:])
        place = pos_v[pl.ds(k, 1), :].astype(jnp.int32)
        column = jnp.sum(jnp.where(lax.broadcasted_iota(jnp.int32, dg_cols.shape, 1) == k, dg_cols, 0.0), axis=1, keepdims=True)
        got = jnp.sum(jnp.where(place == place_iota, column, 0.0), axis=0, keepdims=True)
        kept = jnp.where(place < cap, place + k * cap, -1)
        for j in range(2):
            mine = own_ref[j:j + 1, :] == k
            dgate[j] = jnp.where(mine, got, dgate[j])
            slot[j] = jnp.where(mine, kept, slot[j])
        span = pl.ds(pl.multiple_of(k * cap, cap), cap)
        rows_v[span, :] = jnp.where(row_iota < n_sm[mb, k], rows_v[span, :].astype(F32), 0.0).astype(BF16)
        return (*dgate, *slot)

    zero, none = jnp.zeros((1, tokens), F32), jnp.full((1, tokens), -1, jnp.int32)
    out = lax.fori_loop(0, owners, one, (zero, zero, none, none))
    dgate, slot = out[:2], out[2:]
    dgate_ref[0:1, :] = dgate[0]
    dgate_ref[1:2, :] = dgate[1]
    slots_v[...] = jnp.concatenate([s.astype(F32) for s in slot] + [jnp.zeros((6, tokens), F32)], axis=0).T.astype(jnp.int32)
    step = 256

    def part(i, c):
        here = pl.ds(pl.multiple_of(i * step, step), step)
        iota = lax.broadcasted_iota(jnp.int32, (step, owners * cap), 1)
        hit = (slots_v[here, 0:1] == iota) | (slots_v[here, 1:2] == iota)
        pick = jnp.where(hit, 1.0, 0.0).astype(BF16)
        dx_ref[here, :] = jnp.dot(pick, rows_v[...], preferred_element_type=F32).astype(BF16)
        return c

    lax.fori_loop(0, tokens // step, part, 0)


def combine(n_kept, own_t, backs, dg_back, cap):
    rows, d = backs[0].shape
    micro, _, tokens = own_t.shape
    owners = rows // cap
    whole = pl.BlockSpec(memory_space=pl.ANY)
    pair = pl.BlockSpec((None, 2, tokens), lambda i: (i, 0, 0))
    return pl.pallas_call(
        functools.partial(combine_kernel, owners, cap),
        grid=(micro,),
        in_specs=[pl.BlockSpec(memory_space=pltpu.SMEM), pair, pl.BlockSpec((None, owners, cap), lambda i: (i, 0, 0))] + [whole] * micro,
        out_specs=[pl.BlockSpec((None, tokens, d), lambda i: (i, 0, 0)), pair],
        out_shape=[jax.ShapeDtypeStruct((micro, tokens, d), BF16), jax.ShapeDtypeStruct((micro, 2, tokens), F32)],
        scratch_shapes=[pltpu.VMEM((rows, d), BF16), pltpu.VMEM((tokens, 8), jnp.int32), pltpu.VMEM((owners, tokens), F32), pltpu.SemaphoreType.DMA],
        compiler_params=pltpu.CompilerParams(vmem_limit_bytes=60 * 2**20),
        cost_estimate=pl.CostEstimate(flops=2 * micro * rows * tokens * d, bytes_accessed=12 * 2**20, transcendentals=0),
        name='combine')(n_kept, own_t, dg_back, *backs)


def solution(mesh):
    side = round(mesh.shape['fsdp'] ** (1 / 3))
    cores = mesh.shape['ep']
    grid_mesh = Mesh(mesh.devices.reshape(side, side, side, cores), ('z', 'y', 'x', 'c'))
    tok_spec = P(None, ('z', 'y', 'x', 'c'), None)
    spec_edf = P('c', ('z', 'y', 'x'), None)
    spec_efd = P('c', None, ('z', 'y', 'x'))
    ring = ('x', 'c')

    def local_step(x_in, dy_out, expert_idx, gate_prob, w_one, w_two, w_three):
        micro_count, tok_rows, d_model = x_in.shape
        top_k = expert_idx.shape[2]
        local_experts, shard, ff = w_one.shape
        experts = local_experts * cores
        cap = capacity_of(tok_rows, top_k, experts)
        rows = experts * cap
        ids_t = jnp.transpose(expert_idx, (0, 2, 1))
        own_t = (ids_t % local_experts) * cores + ids_t // local_experts
        q_t = jnp.transpose(gate_prob, (0, 2, 1))
        here = lax.axis_index('x') * cores + lax.axis_index('c')
        mine = jnp.concatenate([own_t.astype(F32), q_t], axis=1)
        tables = [mine]
        for k in range(1, experts):
            tables.append(lax.ppermute(mine, ring, [(i, (i + k) % experts) for i in range(experts)]))
        table = jnp.stack(tables, axis=1).reshape(micro_count * experts, 2 * top_k, tok_rows)
        source = jnp.arange(experts, dtype=jnp.int32)
        is_from = (here - source[:, None]) % experts == source[None, :]
        n_here = jnp.sum((table[:, :top_k] == here.astype(F32)).astype(jnp.int32), axis=(1, 2)).reshape(micro_count, 1, experts)
        n_here = jnp.sum(jnp.where(is_from, n_here, 0), axis=2)
        n_recv = (jnp.minimum(n_here, cap) + UNIT - 1) // UNIT
        picks = (own_t[:, :, :, None] == jnp.arange(experts, dtype=jnp.int32)).astype(jnp.int32)
        n_kept = jnp.minimum(jnp.sum(picks, axis=(1, 2)), cap)
        w_cat = jnp.concatenate([w_one, jnp.transpose(w_two, (0, 2, 1)), w_three], axis=2)
        x_id = lax.axis_index('x')

        def deal(slabs):
            dealt = [lax.dynamic_index_in_dim(slabs, x_id, 0, keepdims=False)]
            for k in range(1, local_experts):
                piece = lax.dynamic_index_in_dim(slabs, (x_id + k) % local_experts, 0, keepdims=False)
                dealt.append(lax.ppermute(piece, 'x', [(i, (i + k) % local_experts) for i in range(local_experts)]))
            result = []
            for j in range(local_experts):
                back = (x_id - j) % local_experts
                slab = dealt[0]
                for k in range(1, local_experts):
                    slab = jnp.where(back == k, dealt[k], slab)
                result.append(slab)
            return result

        w_mine = jnp.concatenate(deal(w_cat), axis=0)
        w_full = lax.all_gather(w_mine, ('z', 'y'), axis=0, tiled=True)
        xdy = []
        for mb in range(micro_count):
            send = dispatch(own_t, x_in, dy_out, mb, experts, cap)
            xdy.append(lax.all_to_all(send.reshape(experts, cap, 2 * d_model), ring, 0, 0, tiled=True).reshape(rows, 2 * d_model))
        gate_rows = slot_gates(here.reshape(1), table, cap).reshape(micro_count, 1, experts, cap)
        gate_rows = jnp.sum(jnp.where(is_from[:, :, None], gate_rows, 0.0), axis=2)
        dx_back = []
        dg_rows = []
        grad_sum = None
        for mb in range(micro_count):
            dx_rows, dg, grad_sum = expert_pass(n_recv[mb], xdy[mb], gate_rows[mb], w_full, grad_sum)
            dx_back.append(lax.all_to_all(dx_rows.reshape(experts, cap, d_model), ring, 0, 0, tiled=True).reshape(rows, d_model))
            dg_rows.append(dg)
        dw_mine = lax.psum_scatter(grad_sum, ('z', 'y'), scatter_dimension=0, tiled=True)
        dg_back = lax.all_to_all(jnp.stack(dg_rows, axis=1), ring, 0, 0, tiled=True)
        done = combine(n_kept, own_t, dx_back, jnp.transpose(dg_back, (1, 0, 2)), cap)
        dx_in, d_gate = done[0], jnp.transpose(done[1], (0, 2, 1))
        dw_all = jnp.stack(deal(dw_mine.reshape(local_experts, shard, 3 * ff)))
        dw_one, dw_two, dw_three = dw_all[:, :, :ff], jnp.transpose(dw_all[:, :, ff:2 * ff], (0, 2, 1)), dw_all[:, :, 2 * ff:]
        return dx_in, d_gate, dw_one, dw_two, dw_three

    return jax.shard_map(local_step, mesh=grid_mesh, in_specs=(tok_spec, tok_spec, tok_spec, tok_spec, spec_edf, spec_efd, spec_edf), out_specs=(tok_spec, tok_spec, spec_edf, spec_efd, spec_edf), check_vma=False)
```

```python
import functools

import jax
import jax.numpy as jnp
from jax import lax
from jax.experimental import pallas as pl
from jax.experimental.pallas import tpu as pltpu
from jax.sharding import Mesh, PartitionSpec as P


F32 = jnp.float32
BF16 = jnp.bfloat16
UNIT = 16
COL_TILE = 256
NT_DIMS = (((1,),(1,)),((),()))


def row_pieces(n_sm, cap, emit):
    off = jnp.int32(0)
    for s in range(n_sm.shape[0]):
        n = n_sm[s]
        for k in range(cap // 64):
            @pl.when((k + 1) * 4 <= n)
            def _(k=k, s=s, off=off):
                emit(s, k * 64, off * UNIT + k * 64, 64)
        base = (n // 4) * 4

        @pl.when((n // 2) % 2 == 1)
        def _(s=s, off=off, base=base):
            emit(s, base * UNIT, (off + base) * UNIT, 32)

        tail = (n // 2) * 2

        @pl.when(n % 2 == 1)
        def _(s=s, off=off, tail=tail):
            emit(s, tail * UNIT, (off + tail) * UNIT, 16)

        off = off + n
    return off


def expert_kernel(ff, cap, first, blocks, n_sm, src_sm, *rest):
    xdy_hbm, (q_ref, w_hbm), rest = rest[:blocks], rest[blocks:blocks + 2], rest[blocks + 2:]
    if first:
        dx_hbm, dg_ref, gw_hbm, xdy_v, q_v, dg_v, dx_v, w_v, gw_v, xt_v, gt_v, sems = rest
        gin_hbm = gin_v = None
    else:
        gin_hbm, dx_hbm, dg_ref, gw_hbm, xdy_v, q_v, dg_v, dx_v, w_v, gw_v, xt_v, gt_v, gin_v, sems = rest
    d = w_hbm.shape[0]
    n_src = n_sm.shape[0]

    def m8(v, n=UNIT):
        return v if isinstance(v, int) else pl.multiple_of(v, n)

    def fetch(s, row, packed, size):
        source, row = (xdy_hbm[0], s * cap + row) if blocks == 1 else (xdy_hbm[s], row)
        return pltpu.make_async_copy(source.at[pl.ds(m8(row), size)], xdy_v.at[pl.ds(m8(packed), size)], sems.at[0])

    units = row_pieces(n_sm, cap, lambda *a: fetch(*a).start())
    parts = [pltpu.make_async_copy(w_hbm.at[:, pl.ds(k * ff, ff)], w_v.at[:, pl.ds(k * ff, ff)], sems.at[1 + k]) for k in range(3)]
    for p in parts:
        p.start()
    if not first:
        gin = pltpu.make_async_copy(gin_hbm, gin_v, sems.at[4])
        gin.start()
    gw_v[...] = jnp.zeros_like(gw_v)
    q_cols = q_ref[...].T
    off = jnp.int32(0)
    for s in range(n_src):
        q_v[pl.ds(pl.multiple_of(off * UNIT, UNIT), cap), :] = q_cols[:, s:s + 1]
        off = off + n_sm[s]
    q_v[pl.ds(pl.multiple_of(off * UNIT, UNIT), 512), :] = jnp.zeros((512, 1), F32)

    def clear(i, c):
        xdy_v[pl.ds(pl.multiple_of(i * UNIT, UNIT), UNIT), :] = jnp.zeros((UNIT, 2 * d), BF16)
        return c

    lax.fori_loop(units, ((units + 31) // 32) * 32, clear, 0)
    row_pieces(n_sm, cap, lambda *a: fetch(*a).wait())
    for p in parts:
        p.wait()

    dot = functools.partial(jnp.dot, preferred_element_type=F32)
    dot_nt = lambda a, b: lax.dot_general(a, b, NT_DIMS, preferred_element_type=F32)

    def tile(lo_row, rt):
        rows = pl.ds(pl.multiple_of(lo_row, 256), rt)
        x = xdy_v[rows, :d]
        dy = xdy_v[rows, d:]
        g = (q_v[rows, :] * dy.astype(F32)).astype(BF16)
        xt_v[:, :rt] = x.T
        gt_v[:, :rt] = g.T
        y = None
        dx = None
        for lo in range(0, ff, COL_TILE):
            one, two, three = (pl.ds(k * ff + lo, COL_TILE) for k in range(3))
            h_one = dot(x, w_v[:, one])
            h_three = dot(x, w_v[:, three])
            d_act = dot(g, w_v[:, two])
            sigma = jax.nn.sigmoid(h_one)
            silu = h_one * sigma
            act = (silu * h_three).astype(BF16)
            dh_three = (d_act * silu).astype(BF16)
            dh_one = (d_act * h_three * sigma * (1.0 + h_one * (1.0 - sigma))).astype(BF16)
            y_part = dot_nt(act, w_v[:, two])
            dx_part = dot_nt(dh_one, w_v[:, one]) + dot_nt(dh_three, w_v[:, three])
            y = y_part if y is None else y + y_part
            dx = dx_part if dx is None else dx + dx_part
            gw_v[:, one] += dot(xt_v[:, :rt], dh_one)
            gw_v[:, three] += dot(xt_v[:, :rt], dh_three)
            gw_v[:, two] += dot(gt_v[:, :rt], act)
        dg_v[rows, :] = jnp.sum(dy.astype(F32) * y, axis=1, keepdims=True)
        dx_v[rows, :] = dx.astype(BF16)

    total = units * UNIT
    full = (total + 511) // 512

    def big(i, c):
        tile(i * 512, 512)
        return c

    lax.fori_loop(0, full, big, 0)

    if not first:
        gin.wait()
    outs = []
    for k in range(3):
        cols = pl.ds(k * ff, ff)
        if not first:
            gw_v[:, cols] += gin_v[:, cols]
        o = pltpu.make_async_copy(gw_v.at[:, cols], gw_hbm.at[:, cols], sems.at[1 + k])
        o.start()
        outs.append(o)

    def put(s, row, packed, size):
        return pltpu.make_async_copy(dx_v.at[pl.ds(m8(packed), size)], dx_hbm.at[pl.ds(m8(src_sm[s] * cap + row), size)], sems.at[0])

    row_pieces(n_sm, cap, lambda *a: put(*a).start())
    off = jnp.int32(0)
    cols = []
    for s in range(n_src):
        cols.append(dg_v[pl.ds(pl.multiple_of(off * UNIT, UNIT), cap), :])
        off = off + n_sm[s]
    dg_ref[...] = jnp.concatenate(cols, axis=1).T
    row_pieces(n_sm, cap, lambda *a: put(*a).wait())
    for o in outs:
        o.wait()


def expert_pass(n_units, sources, xdy, gates, w_full, grad_in):
    d2 = xdy[0].shape[1]
    rows = sum(block.shape[0] for block in xdy)
    d = d2 // 2
    ff = w_full.shape[1] // 3
    cap = gates.shape[1]
    first = grad_in is None
    whole = pl.BlockSpec(memory_space=pl.ANY)
    vm = pl.BlockSpec(memory_space=pltpu.VMEM)
    args = [n_units, sources, *xdy, gates, w_full] + ([] if first else [grad_in])
    smem = pl.BlockSpec(memory_space=pltpu.SMEM)
    in_specs = [smem, smem] + [whole] * len(xdy) + [vm, whole] + ([] if first else [whole])
    pad = rows + 512
    scratch = [
        pltpu.VMEM((rows, d2), BF16), pltpu.VMEM((pad, 1), F32), pltpu.VMEM((pad, 1), F32), pltpu.VMEM((rows, d), BF16),
        pltpu.VMEM((d, 3 * ff), BF16), pltpu.VMEM((d, 3 * ff), F32), pltpu.VMEM((d, 512), BF16), pltpu.VMEM((d, 512), BF16)]
    if not first:
        scratch.append(pltpu.VMEM((d, 3 * ff), F32))
    scratch.append(pltpu.SemaphoreType.DMA((5,)))
    return pl.pallas_call(
        functools.partial(expert_kernel, ff, cap, first, len(xdy)),
        in_specs=in_specs, out_specs=[whole, vm, whole],
        out_shape=[jax.ShapeDtypeStruct((rows, d), BF16), jax.ShapeDtypeStruct(gates.shape, F32), jax.ShapeDtypeStruct((d, 3 * ff), F32)],
        scratch_shapes=scratch,
        compiler_params=pltpu.CompilerParams(vmem_limit_bytes=60 * 2**20),
        cost_estimate=pl.CostEstimate(flops=18 * rows * d * ff, bytes_accessed=40 * 2**20, transcendentals=2 * rows * ff),
        name='expert_first' if first else 'expert_next')(*args)


def capacity_of(tok_rows, top_k, experts):
    return 8 * ((5 * tok_rows * top_k + 32 * experts - 1) // (32 * experts))


def positions(own_ref, owners):
    tokens = own_ref.shape[1]
    who = lax.broadcasted_iota(jnp.int32, (owners, tokens), 0)
    chosen = (own_ref[0:1, :] == who) | (own_ref[1:2, :] == who)
    before = lax.broadcasted_iota(jnp.int32, (tokens, tokens), 0) < lax.broadcasted_iota(jnp.int32, (tokens, tokens), 1)
    flags = jnp.where(chosen, 1.0, 0.0).astype(BF16)
    place = jnp.dot(flags, jnp.where(before, 1.0, 0.0).astype(BF16), preferred_element_type=F32)
    return jnp.where(chosen, place, -1.0)


def dispatch_kernel(owners, cap, own_ref, x_ref, dy_ref, xdy_ref, pos_v):
    step = pl.program_id(0)
    d = x_ref.shape[1]

    @pl.when(step == 0)
    def _():
        pos_v[...] = positions(own_ref, owners)

    place = pos_v[pl.ds(step, 1), :].astype(jnp.int32)
    hit = place == lax.broadcasted_iota(jnp.int32, (cap, place.shape[1]), 0)
    pick = jnp.where(hit, 1.0, 0.0).astype(BF16)
    xdy_ref[:, :d] = jnp.dot(pick, x_ref[...], preferred_element_type=F32).astype(BF16)
    xdy_ref[:, d:] = jnp.dot(pick, dy_ref[...], preferred_element_type=F32).astype(BF16)


def dispatch(own_t, x_in, dy_out, mb, owners, cap):
    _, tokens, d = x_in.shape
    part = pl.BlockSpec((None, tokens, d), lambda i: (mb, 0, 0))
    return pl.pallas_call(
        functools.partial(dispatch_kernel, owners, cap),
        grid=(owners,),
        in_specs=[pl.BlockSpec((None, 2, tokens), lambda i: (mb, 0, 0)), part, part],
        out_specs=pl.BlockSpec((cap, 2 * d), lambda i: (i, 0)),
        out_shape=jax.ShapeDtypeStruct((owners * cap, 2 * d), BF16),
        scratch_shapes=[pltpu.VMEM((owners, tokens), F32)],
        compiler_params=pltpu.CompilerParams(vmem_limit_bytes=60 * 2**20),
        cost_estimate=pl.CostEstimate(flops=4 * owners * cap * tokens * d, bytes_accessed=8 * 2**20, transcendentals=0))(own_t, x_in, dy_out)


def gates_kernel(cap, here_sm, table_ref, gate_ref, cols_v, place_v, gate_v):
    blocks, tokens = table_ref.shape[0], table_ref.shape[2]
    here = here_sm[0].astype(F32)
    row = lambda j: jnp.concatenate([table_ref[k, j:j + 1, :] for k in range(blocks)], axis=0)
    first = row(0) == here
    chosen = first | (row(1) == here)
    before = lax.broadcasted_iota(jnp.int32, (tokens, tokens), 0) < lax.broadcasted_iota(jnp.int32, (tokens, tokens), 1)
    flags = jnp.where(chosen, 1.0, 0.0).astype(BF16)
    place = jnp.dot(flags, jnp.where(before, 1.0, 0.0).astype(BF16), preferred_element_type=F32)
    place_v[...] = jnp.where(chosen, place, -1.0).astype(jnp.int32)
    gate_v[...] = jnp.where(first, row(2), row(3))
    cols_v[...] = jnp.zeros_like(cols_v)

    def one(k, c):
        hit = place_v[pl.ds(k, 1), :] == lax.broadcasted_iota(jnp.int32, (cap, tokens), 0)
        column = jnp.sum(jnp.where(hit, gate_v[pl.ds(k, 1), :], 0.0), axis=1, keepdims=True)
        cols_v[...] += jnp.where(lax.broadcasted_iota(jnp.int32, cols_v.shape, 1) == k, column, 0.0)
        return c

    lax.fori_loop(0, blocks, one, 0)
    gate_ref[...] = cols_v[...].T[:blocks, :]


def slot_gates(here, table, cap):
    blocks, _, tokens = table.shape
    vm = pl.BlockSpec(memory_space=pltpu.VMEM)
    return pl.pallas_call(
        functools.partial(gates_kernel, cap),
        in_specs=[pl.BlockSpec(memory_space=pltpu.SMEM), vm],
        out_specs=vm,
        out_shape=jax.ShapeDtypeStruct((blocks, cap), F32),
        scratch_shapes=[pltpu.VMEM((cap, 128), F32), pltpu.VMEM((blocks, tokens), jnp.int32), pltpu.VMEM((blocks, tokens), F32)],
        cost_estimate=pl.CostEstimate(flops=10 * 2**30, bytes_accessed=2**20, transcendentals=0),
        name='slot_gates')(here, table)


def combine_kernel(owners, cap, n_sm, own_ref, dg_ref, *rest):
    backs, (dx_ref, dgate_ref, rows_v, slots_v, pos_v, sem) = rest[:-6], rest[-6:]
    mb = pl.program_id(0)
    for k, back in enumerate(backs):
        @pl.when(mb == k)
        def _(back=back):
            copy = pltpu.make_async_copy(back, rows_v, sem)
            copy.start()
            copy.wait()
    tokens = own_ref.shape[1]
    d = rows_v.shape[1]
    pos_v[...] = positions(own_ref, owners)
    dg_cols = dg_ref[...].T
    place_iota = lax.broadcasted_iota(jnp.int32, (cap, tokens), 0)
    row_iota = lax.broadcasted_iota(jnp.int32, (cap, d), 0)

    def one(k, c):
        dgate, slot = list(c[:2]), list(c[2:])
        place = pos_v[pl.ds(k, 1), :].astype(jnp.int32)
        column = jnp.sum(jnp.where(lax.broadcasted_iota(jnp.int32, dg_cols.shape, 1) == k, dg_cols, 0.0), axis=1, keepdims=True)
        got = jnp.sum(jnp.where(place == place_iota, column, 0.0), axis=0, keepdims=True)
        kept = jnp.where(place < cap, place + k * cap, -1)
        for j in range(2):
            mine = own_ref[j:j + 1, :] == k
            dgate[j] = jnp.where(mine, got, dgate[j])
            slot[j] = jnp.where(mine, kept, slot[j])
        span = pl.ds(pl.multiple_of(k * cap, cap), cap)
        rows_v[span, :] = jnp.where(row_iota < n_sm[mb, k], rows_v[span, :].astype(F32), 0.0).astype(BF16)
        return (*dgate, *slot)

    zero, none = jnp.zeros((1, tokens), F32), jnp.full((1, tokens), -1, jnp.int32)
    out = lax.fori_loop(0, owners, one, (zero, zero, none, none))
    dgate, slot = out[:2], out[2:]
    dgate_ref[0:1, :] = dgate[0]
    dgate_ref[1:2, :] = dgate[1]
    slots_v[...] = jnp.concatenate([s.astype(F32) for s in slot] + [jnp.zeros((6, tokens), F32)], axis=0).T.astype(jnp.int32)
    step = 256

    def part(i, c):
        here = pl.ds(pl.multiple_of(i * step, step), step)
        iota = lax.broadcasted_iota(jnp.int32, (step, owners * cap), 1)
        hit = (slots_v[here, 0:1] == iota) | (slots_v[here, 1:2] == iota)
        pick = jnp.where(hit, 1.0, 0.0).astype(BF16)
        dx_ref[here, :] = jnp.dot(pick, rows_v[...], preferred_element_type=F32).astype(BF16)
        return c

    lax.fori_loop(0, tokens // step, part, 0)


def combine(n_kept, own_t, backs, dg_back, cap):
    rows, d = backs[0].shape
    micro, _, tokens = own_t.shape
    owners = rows // cap
    whole = pl.BlockSpec(memory_space=pl.ANY)
    pair = pl.BlockSpec((None, 2, tokens), lambda i: (i, 0, 0))
    return pl.pallas_call(
        functools.partial(combine_kernel, owners, cap),
        grid=(micro,),
        in_specs=[pl.BlockSpec(memory_space=pltpu.SMEM), pair, pl.BlockSpec((None, owners, cap), lambda i: (i, 0, 0))] + [whole] * micro,
        out_specs=[pl.BlockSpec((None, tokens, d), lambda i: (i, 0, 0)), pair],
        out_shape=[jax.ShapeDtypeStruct((micro, tokens, d), BF16), jax.ShapeDtypeStruct((micro, 2, tokens), F32)],
        scratch_shapes=[pltpu.VMEM((rows, d), BF16), pltpu.VMEM((tokens, 8), jnp.int32), pltpu.VMEM((owners, tokens), F32), pltpu.SemaphoreType.DMA],
        compiler_params=pltpu.CompilerParams(vmem_limit_bytes=60 * 2**20),
        cost_estimate=pl.CostEstimate(flops=2 * micro * rows * tokens * d, bytes_accessed=12 * 2**20, transcendentals=0),
        name='combine')(n_kept, own_t, dg_back, *backs)


def solution(mesh):
    side = round(mesh.shape['fsdp'] ** (1 / 3))
    cores = mesh.shape['ep']
    grid_mesh = Mesh(mesh.devices.reshape(side, side, side, cores), ('z', 'y', 'x', 'c'))
    tok_spec = P(None, ('z', 'y', 'x', 'c'), None)
    spec_edf = P('c', ('z', 'y', 'x'), None)
    spec_efd = P('c', None, ('z', 'y', 'x'))
    ring = ('x', 'c')

    def local_step(x_in, dy_out, expert_idx, gate_prob, w_one, w_two, w_three):
        micro_count, tok_rows, d_model = x_in.shape
        top_k = expert_idx.shape[2]
        local_experts, shard, ff = w_one.shape
        experts = local_experts * cores
        cap = capacity_of(tok_rows, top_k, experts)
        rows = experts * cap
        ids_t = jnp.transpose(expert_idx, (0, 2, 1))
        own_t = (ids_t % local_experts) * cores + ids_t // local_experts
        q_t = jnp.transpose(gate_prob, (0, 2, 1))
        here = lax.axis_index('x') * cores + lax.axis_index('c')
        mine = jnp.concatenate([own_t.astype(F32), q_t], axis=1)
        tables = [mine]
        for k in range(1, experts):
            tables.append(lax.ppermute(mine, ring, [(i, (i + k) % experts) for i in range(experts)]))
        table = jnp.stack(tables, axis=1).reshape(micro_count * experts, 2 * top_k, tok_rows)
        source = jnp.arange(experts, dtype=jnp.int32)
        is_from = (here - source[:, None]) % experts == source[None, :]
        n_here = jnp.sum((table[:, :top_k] == here.astype(F32)).astype(jnp.int32), axis=(1, 2)).reshape(micro_count, 1, experts)
        n_near = (jnp.minimum(n_here, cap) + UNIT - 1) // UNIT
        n_recv = [jnp.sum(jnp.where(is_from, n_near[0], 0), axis=1), n_near[1, 0]]
        came = [source, (here - source) % experts]
        picks = (own_t[:, :, :, None] == jnp.arange(experts, dtype=jnp.int32)).astype(jnp.int32)
        n_kept = jnp.minimum(jnp.sum(picks, axis=(1, 2)), cap)
        w_cat = jnp.concatenate([w_one, jnp.transpose(w_two, (0, 2, 1)), w_three], axis=2)
        x_id = lax.axis_index('x')

        def deal(slabs):
            dealt = [lax.dynamic_index_in_dim(slabs, x_id, 0, keepdims=False)]
            for k in range(1, local_experts):
                piece = lax.dynamic_index_in_dim(slabs, (x_id + k) % local_experts, 0, keepdims=False)
                dealt.append(lax.ppermute(piece, 'x', [(i, (i + k) % local_experts) for i in range(local_experts)]))
            result = []
            for j in range(local_experts):
                back = (x_id - j) % local_experts
                slab = dealt[0]
                for k in range(1, local_experts):
                    slab = jnp.where(back == k, dealt[k], slab)
                result.append(slab)
            return result

        w_mine = jnp.concatenate(deal(w_cat), axis=0)
        w_full = lax.all_gather(w_mine, ('z', 'y'), axis=0, tiled=True)
        xdy = []
        for mb in range(micro_count):
            send = dispatch(own_t, x_in, dy_out, mb, experts, cap)
            send = send.reshape(experts, cap, 2 * d_model)
            if mb == 0:
                xdy.append([lax.all_to_all(send, ring, 0, 0, tiled=True).reshape(rows, 2 * d_model)])
                continue
            blocks = []
            for k in range(experts):
                block = lax.dynamic_index_in_dim(send, (here + k) % experts, 0, keepdims=False)
                blocks.append(lax.ppermute(block, ring, [(i, (i + k) % experts) for i in range(experts)]) if k else block)
            xdy.append(blocks)
        gate_rows = slot_gates(here.reshape(1), table, cap).reshape(micro_count, experts, cap)
        gate_rows = [jnp.sum(jnp.where(is_from[:, :, None], gate_rows[0], 0.0), axis=1), gate_rows[1]]
        dx_back = []
        dg_rows = []
        grad_sum = None
        for mb in range(micro_count):
            dx_rows, dg, grad_sum = expert_pass(n_recv[mb], came[mb], xdy[mb], gate_rows[mb], w_full, grad_sum)
            dx_back.append(lax.all_to_all(dx_rows.reshape(experts, cap, d_model), ring, 0, 0, tiled=True).reshape(rows, d_model))
            dg_rows.append(dg if mb == 0 else jnp.sum(jnp.where(is_from[:, :, None], dg[None], 0.0), axis=1))
        dw_mine = lax.psum_scatter(grad_sum, ('z', 'y'), scatter_dimension=0, tiled=True)
        dg_back = lax.all_to_all(jnp.stack(dg_rows, axis=1), ring, 0, 0, tiled=True)
        done = combine(n_kept, own_t, dx_back, jnp.transpose(dg_back, (1, 0, 2)), cap)
        dx_in, d_gate = done[0], jnp.transpose(done[1], (0, 2, 1))
        dw_all = jnp.stack(deal(dw_mine.reshape(local_experts, shard, 3 * ff)))
        dw_one, dw_two, dw_three = dw_all[:, :, :ff], jnp.transpose(dw_all[:, :, ff:2 * ff], (0, 2, 1)), dw_all[:, :, 2 * ff:]
        return dx_in, d_gate, dw_one, dw_two, dw_three

    return jax.shard_map(local_step, mesh=grid_mesh, in_specs=(tok_spec, tok_spec, tok_spec, tok_spec, spec_edf, spec_efd, spec_edf), out_specs=(tok_spec, tok_spec, spec_edf, spec_efd, spec_edf), check_vma=False)
```
